32 devices in a mesh: head: 4 (over x, core), blk: 8 (over z, y).
Axes of the slice: x: 2, y: 2, z: 4, core: 2. Of those that a mesh axis runs over, the one named last changes fastest.
Arguments:
- tokens: bfloat16 [4096, 2048], P(('head', 'blk')), may hold values from -6 to 6
- norm1_gain: float32 [2048], replicated, may hold values from 0.5 to 1.5
- norm1_bias: float32 [2048], replicated, may hold values from -3 to 3
- w_qkv: bfloat16 [2048, 3, 2048], P('blk', None, 'head'), may hold values from -0.125 to 0.125
- qkv_bias: float32 [3, 2048], P(None, 'head'), may hold values from -3 to 3
- w_out: bfloat16 [2048, 2048], P('head', 'blk'), may hold values from -0.5 to 0.5
- norm2_gain: float32 [2048], replicated, may hold values from 0.5 to 1.5
- norm2_bias: float32 [2048], replicated, may hold values from -3 to 3
- w_gate: bfloat16 [2048, 5632], P('blk', 'head'), may hold values from -0.125 to 0.125
- w_up: bfloat16 [2048, 5632], P('blk', 'head'), may hold values from -0.125 to 0.125
- w_down: bfloat16 [5632, 2048], P('head', 'blk'), may hold values from -0.078125 to 0.078125
- cotangent: bfloat16 [4096, 2048], P(('head', 'blk')), may hold values from -6 to 6
- seq_lengths: int32 [8], replicated, may hold values from 1 to 2048, 4096 in all
- block_order: int32 [32], replicated, may hold values from 0 to 31, each once
Outputs:
- output: bfloat16 [4096, 2048], P(('head', 'blk'))
- input_grad: float32 [4096, 2048], P(('head', 'blk'))
- norm1_gain_grad: float32 [2048], P(('head', 'blk'))
- norm1_bias_grad: float32 [2048], P(('head', 'blk'))
- w_qkv_grad: float32 [2048, 3, 2048], P('blk', None, 'head')
- qkv_bias_grad: float32 [3, 2048], P(None, ('head', 'blk'))
- w_out_grad: float32 [2048, 2048], P('head', 'blk')
- norm2_gain_grad: float32 [2048], P(('head', 'blk'))
- norm2_bias_grad: float32 [2048], P(('head', 'blk'))
- w_gate_grad: float32 [2048, 5632], P('blk', 'head')
- w_up_grad: float32 [2048, 5632], P('blk', 'head')
- w_down_grad: float32 [5632, 2048], P('head', 'blk')
The draws below stay inside these ranges and needn't reach their ends.
Inputs may be any that keep to these rules, and one draw needn't show every extreme that they name: `seq_lengths`: 8 sequences lie end to end over the packed positions 0 to 4095 in this order; the longest has exactly 2048 tokens. Each block number appears once; rows j * 128 to j * 128 + 127 of tokens and cotangent are packed block block_order[j].
All inputs are finite; a program needn't handle non-finite values.
Results may differ from the reference program's by a relative error of at most 0.019.
Values may be sent and summed in bfloat16 or wider, within the bound.
A program may use at most 320 MiB of HBM per device.

```python
import math
import jax
import jax.numpy as jnp
import numpy as np
from jax import lax

D = 2048
HEADS = 32
HD = 64
ROT = 16
FF = 5632
BLOCK = 128
NSEQ = 8
TOKENS = 4096
NBLOCKS = 32
LONGEST = 2048


def shard_levels(key, dims, cuts, least, largest):
    gain = 1.0
    for dim, shards_of in cuts:
        steps = jax.random.uniform(jax.random.fold_in(jax.random.fold_in(key, 6), dim), (shards_of,), jnp.float32, least / len(cuts), largest / len(cuts))
        gain = gain * jnp.repeat(jnp.exp(steps), dims[dim] // shards_of).reshape((-1,) + (1,) * (len(dims) - 1 - dim))
    return gain


def profile(number_of, total, most, slope):
    loads = [(1 << 20) // math.isqrt(rank ** slope) + 1 for rank in range(2, number_of + 1)]
    spare, holding = total - most - (number_of - 1), [1] * (number_of - 1)
    while spare > 0:
        free = [i for i in range(number_of - 1) if holding[i] < most]
        whole, remaining = sum([loads[i] for i in free]), spare
        for i in free:
            more = min(most - holding[i], max(1, remaining * loads[i] // whole), spare)
            holding[i] = holding[i] + more
            spare = spare - more
    return np.array([most] + holding)


def ragged(key, number_of, total, most, lean):
    if number_of == 2:
        one = jax.random.randint(key, (), max(1, total - most), min(most, total - 1) + 1)
        return jnp.stack([one, total - one])
    lengths = jnp.asarray(profile(number_of, total, most, lean), jnp.int32)
    pairs = (number_of - 1) // 2
    source_of, receiver = lengths[1:1 + 2 * pairs:2], lengths[2:2 + 2 * pairs:2]
    margin = jnp.minimum(source_of - 1, most - receiver)
    moved = jax.random.randint(jax.random.fold_in(key, 1), (pairs,), 0, 1 << 20) % (margin + 1)
    lengths = lengths.at[1:1 + 2 * pairs:2].set(source_of - moved).at[2:2 + 2 * pairs:2].set(receiver + moved)
    return lengths[jax.random.permutation(jax.random.fold_in(key, 2), number_of)]


def noise(own_key, dims, deviation, limit, cuts=(), kind=jnp.bfloat16):
    values = deviation * jax.random.normal(own_key, dims, jnp.float32)
    if cuts:
        values = values * shard_levels(own_key, dims, cuts, -0.22, 0.18)
    return jnp.clip(values, -limit, limit).astype(kind)


def setup_inputs(seed: int = 0) -> dict:
    arg_keys = jax.random.split(jax.random.key(seed), 15)
    return {
        "tokens": noise(arg_keys[0], (TOKENS, D), 1.0, 6.0, ((0, 32),)),
        "norm1_gain": jnp.clip(1.0 + 0.1 * jax.random.normal(arg_keys[1], (D,), jnp.float32), 0.5, 1.5),
        "norm1_bias": noise(arg_keys[2], (D,), 0.5, 3.0, (), jnp.float32),
        "w_qkv": noise(arg_keys[3], (D, 3, D), D ** -0.5, 0.125, ((0, 8), (2, 4))),
        "qkv_bias": noise(arg_keys[4], (3, D), 0.5, 3.0, ((1, 4),), jnp.float32),
        "w_out": noise(arg_keys[5], (D, D), (D // 16) ** -0.5, 0.5, ((0, 4), (1, 8))),
        "norm2_gain": jnp.clip(1.0 + 0.1 * jax.random.normal(arg_keys[6], (D,), jnp.float32), 0.5, 1.5),
        "norm2_bias": noise(arg_keys[7], (D,), 0.5, 3.0, (), jnp.float32),
        "w_gate": noise(arg_keys[8], (D, FF), D ** -0.5, 0.125, ((0, 8), (1, 4))),
        "w_up": noise(arg_keys[9], (D, FF), D ** -0.5, 0.125, ((0, 8), (1, 4))),
        "w_down": noise(arg_keys[10], (FF, D), FF ** -0.5, 0.078125, ((0, 4), (1, 8))),
        "cotangent": noise(arg_keys[11], (TOKENS, D), 1.0, 6.0, ((0, 32),)),
        "seq_lengths": ragged(arg_keys[12], NSEQ, TOKENS, LONGEST, 2).astype(jnp.int32),
        "block_order": jax.random.permutation(arg_keys[13], NBLOCKS).astype(jnp.int32),
    }


@jax.custom_vjp
def low(v):
    return lax.optimization_barrier(v.astype(jnp.bfloat16)).astype(jnp.float32)

@jax.custom_vjp
def low_back(v):
    return v

def low_keep(v):
    return (low(v), None)

def low_pass(kept, grad):
    return (grad,)

def back_keep(v):
    return (v, None)

def back_low(kept, grad):
    return (low(grad),)
low.defvjp(low_keep, low_pass)
low_back.defvjp(back_keep, back_low)
EPSILON = 1e-05
MASKED = -1000000000.0
HIGH = lax.Precision.HIGHEST

def layer_norm(values, norm_gain, norm_shift):
    centre = values - lax.optimization_barrier(jnp.mean(values, axis=-1, keepdims=True))
    inv_scale = lax.rsqrt(lax.optimization_barrier(jnp.mean(centre * centre, axis=-1, keepdims=True)) + EPSILON)
    return centre * inv_scale * norm_gain + norm_shift

def rotate(values, cosine, sine_table):
    half_rot = ROT // 2
    lead_part = values[..., :half_rot]
    tail_part = values[..., half_rot:ROT]
    cos_rows = cosine[:, None, :]
    sin_rows = sine_table[:, None, :]
    return jnp.concatenate([lead_part * cos_rows - tail_part * sin_rows, tail_part * cos_rows + lead_part * sin_rows, values[..., ROT:]], axis=-1)

def reference(tokens, norm1_gain, norm1_bias, w_qkv, qkv_bias, w_out, norm2_gain, norm2_bias, w_gate, w_up, w_down, cotangent, seq_lengths, block_order):
    row_total = TOKENS
    rows_all = jnp.arange(row_total, dtype=jnp.int32)
    position = (block_order[rows_all // BLOCK] * BLOCK + rows_all % BLOCK).astype(jnp.int32)
    seq_ends = jnp.cumsum(seq_lengths)
    seq_start = lax.optimization_barrier(jnp.sum(jnp.where(seq_ends[None, :] <= position[:, None], seq_lengths[None, :], 0), axis=1)).astype(jnp.int32)
    half_rot = ROT // 2
    freq_table = jnp.power(10000.0, -2.0 * jnp.arange(half_rot, dtype=jnp.float32) / ROT)
    angles = (position - seq_start).astype(jnp.float32)[:, None] * freq_table[None, :]
    cosine = jnp.cos(angles)
    sine_table = jnp.sin(angles)
    scale = HD ** (-0.5)
    query_block = 128
    block_count = row_total // query_block

    def forward(tokens_f, gain_one, shift_one, qkv_weight, qkv_shift, out_weight, gain_two, shift_two, gate_weight, up_weight, down_weight):
        norm1 = low(layer_norm(tokens_f, gain_one, shift_one))
        proj = jnp.dot(norm1, qkv_weight.reshape(D, 3 * D), precision=HIGH).reshape(row_total, 3, D) + qkv_shift[None]
        proj = low_back(proj).reshape(row_total, 3, HEADS, HD)
        queries = low(rotate(proj[:, 0], cosine, sine_table))
        keys = low(rotate(proj[:, 1], cosine, sine_table))
        values = low(proj[:, 2])

        def one_block(item_args):
            q_tile, pos_tile, start_tile = item_args
            raw_scores = jnp.einsum('qhd,khd->hqk', q_tile, keys, precision=HIGH) * scale
            allowed = (position[None, :] <= pos_tile[:, None]) & (position[None, :] >= start_tile[:, None])
            scores = low_back(jnp.where(allowed[None], raw_scores, MASKED))
            row_max = lax.optimization_barrier(jnp.max(scores, axis=-1, keepdims=True))
            exp_scores = jnp.exp(scores - row_max)
            probs_f32 = exp_scores / lax.optimization_barrier(jnp.sum(exp_scores, axis=-1, keepdims=True))
            return jnp.einsum('hqk,khd->qhd', low(probs_f32), values, precision=HIGH)
        attended = lax.map(jax.checkpoint(one_block), (queries.reshape(block_count, query_block, HEADS, HD), position.reshape(block_count, query_block), seq_start.reshape(block_count, query_block)))
        attn = low(low_back(attended.reshape(row_total, D)))
        hidden = tokens_f + low_back(jnp.dot(attn, out_weight, precision=HIGH))
        norm2 = low(layer_norm(hidden, gain_two, shift_two))
        gate_val = low_back(jnp.dot(norm2, gate_weight, precision=HIGH))
        up_val = low_back(jnp.dot(norm2, up_weight, precision=HIGH))
        activ = low(jax.nn.silu(gate_val) * up_val)
        return hidden + low_back(jnp.dot(activ, down_weight, precision=HIGH))
    inputs = (tokens.astype(jnp.float32), norm1_gain.astype(jnp.float32), norm1_bias.astype(jnp.float32), w_qkv.astype(jnp.float32), qkv_bias.astype(jnp.float32), w_out.astype(jnp.float32), norm2_gain.astype(jnp.float32), norm2_bias.astype(jnp.float32), w_gate.astype(jnp.float32), w_up.astype(jnp.float32), w_down.astype(jnp.float32))
    result, pull_back = jax.vjp(forward, *inputs)
    grads = pull_back(cotangent.astype(jnp.float32))
    return (result.astype(jnp.bfloat16), grads[0], grads[1], grads[2], grads[3], grads[4], grads[5], grads[6], grads[7], grads[8], grads[9], grads[10])
```

```python
import jax
import jax.numpy as jnp
from jax import lax
from jax.experimental import pallas as pl
from jax.experimental.pallas import tpu as pltpu
from jax.sharding import PartitionSpec as P

HD = 64
ROT = 16
BLOCK = 128
Z_PARTS = 4
QUERY_TILE = 512
KEY_TILE = 256


EPSILON = 1e-05
MASKED = -1000000000.0


def contract_rows(left, right):
    return lax.dot_general(
        left, right, (((0,), (0,)), ((), ())), preferred_element_type=jnp.float32
    )


def times_transpose(left, right):
    return lax.dot_general(
        left, right, (((1,), (1,)), ((), ())), preferred_element_type=jnp.float32
    )


def packed_positions(row_ids, block_order):
    block_ids = jnp.arange(block_order.shape[0], dtype=jnp.int32)
    matches = (row_ids // BLOCK)[:, None] == block_ids[None, :]
    block_start = jnp.sum(jnp.where(matches, block_order[None, :], 0), axis=1)
    return block_start * BLOCK + row_ids % BLOCK


def sequence_start(position, seq_lengths):
    seq_ends = jnp.cumsum(seq_lengths)
    ends_before = seq_ends[None, :] <= position[:, None]
    return jnp.sum(jnp.where(ends_before, seq_lengths[None, :], 0), axis=1)


def rotate(values, cosine, sine_table):
    half_rot = ROT // 2
    lead_part = values[..., :half_rot]
    tail_part = values[..., half_rot:ROT]
    cos_rows = cosine[:, None, :]
    sin_rows = sine_table[:, None, :]
    return jnp.concatenate(
        [
            lead_part * cos_rows - tail_part * sin_rows,
            tail_part * cos_rows + lead_part * sin_rows,
            values[..., ROT:],
        ],
        axis=-1,
    )


def normalize(values, norm_gain, norm_shift):
    centre = values - jnp.mean(values, axis=-1, keepdims=True)
    inv_scale = lax.rsqrt(jnp.mean(centre * centre, axis=-1, keepdims=True) + EPSILON)
    unit_rows = centre * inv_scale
    return (unit_rows * norm_gain + norm_shift, unit_rows, inv_scale)


def normalize_back(grad_norm, unit_rows, inv_scale, norm_gain):
    grad_unit = grad_norm * norm_gain
    mean_grad = jnp.mean(grad_unit, axis=-1, keepdims=True)
    mean_proj = jnp.mean(grad_unit * unit_rows, axis=-1, keepdims=True)
    return inv_scale * (grad_unit - mean_grad - unit_rows * mean_proj)


def gather_keys(keys_flat, values_flat):
    return (
        lax.all_gather(keys_flat, "blk", axis=0, tiled=True),
        lax.all_gather(values_flat, "blk", axis=0, tiled=True),
    )


def tile_count_of(total_rows):
    tile_rows = min(1024, total_rows)
    return (total_rows // tile_rows, tile_rows)


def key_tiles(keys_all, values_all, key_pos, heads_local):
    tile_count, tile_rows = tile_count_of(keys_all.shape[0])
    return (
        keys_all.reshape(tile_count, tile_rows, heads_local, HD),
        values_all.reshape(tile_count, tile_rows, heads_local, HD),
        key_pos.reshape(tile_count, tile_rows),
    )


def masked_scores(queries, key_tile, pos_tile, query_pos, query_start):
    raw_scores = jnp.einsum(
        "qhd,khd->hqk", queries, key_tile, preferred_element_type=jnp.float32
    ) * HD ** (-0.5)
    allowed = (pos_tile[None, :] <= query_pos[:, None]) & (
        pos_tile[None, :] >= query_start[:, None]
    )
    return jnp.where(allowed[None], raw_scores, MASKED)


def attend(queries, tiles, query_pos, query_start):
    group_rows = queries.shape[0]
    heads_local = queries.shape[1]

    def first_pass(run_state, tile):
        run_max, run_sum = run_state
        scores = masked_scores(queries, tile[0], tile[2], query_pos, query_start)
        new_max = jnp.maximum(run_max, jnp.max(scores, axis=-1))
        new_sum = run_sum * jnp.exp(run_max - new_max) + jnp.sum(
            jnp.exp(scores - new_max[..., None]), axis=-1
        )
        return ((new_max, new_sum), None)

    start_state = (
        jnp.full((heads_local, group_rows), -3e38, jnp.float32),
        jnp.zeros((heads_local, group_rows), jnp.float32),
    )
    (run_max, run_sum), unused = lax.scan(first_pass, start_state, tiles)
    log_norm = run_max + jnp.log(run_sum)

    def second_pass(totals, tile):
        total_out, total_rest = totals
        scores = masked_scores(queries, tile[0], tile[2], query_pos, query_start)
        probs_f32 = jnp.exp(scores - log_norm[..., None])
        probs_b = probs_f32.astype(jnp.bfloat16)
        rest_b = (probs_f32 - probs_b.astype(jnp.float32)).astype(jnp.bfloat16)
        total_out = total_out + jnp.einsum(
            "hqk,khd->qhd", probs_b, tile[1], preferred_element_type=jnp.float32
        )
        total_rest = total_rest + jnp.einsum(
            "hqk,khd->qhd", rest_b, tile[1], preferred_element_type=jnp.float32
        )
        return ((total_out, total_rest), None)

    empty = jnp.zeros((group_rows, heads_local, HD), jnp.float32)
    (attended, leftover), unused = lax.scan(second_pass, (empty, empty), tiles)
    return (attended, attended + leftover, log_norm)


def attend_back(queries, tiles, query_pos, query_start, log_norm, grad_attn, delta_rows):
    scale = HD ** (-0.5)

    def step_back(grad_query, tile):
        key_tile, value_tile, pos_tile = tile
        scores = masked_scores(queries, key_tile, pos_tile, query_pos, query_start)
        probs_f32 = jnp.exp(scores - log_norm[..., None])
        grad_probs = jnp.einsum(
            "qhd,khd->hqk", grad_attn, value_tile, preferred_element_type=jnp.float32
        )
        grad_scores = (probs_f32 * (grad_probs - delta_rows[..., None])).astype(jnp.bfloat16)
        probs_b = probs_f32.astype(jnp.bfloat16)
        grad_query = grad_query + scale * jnp.einsum(
            "hqk,khd->qhd", grad_scores, key_tile, preferred_element_type=jnp.float32
        )
        grad_key = scale * jnp.einsum(
            "hqk,qhd->khd", grad_scores, queries, preferred_element_type=jnp.float32
        )
        grad_value = jnp.einsum(
            "hqk,qhd->khd", probs_b, grad_attn, preferred_element_type=jnp.float32
        )
        return (grad_query, (grad_key, grad_value))

    grad_query, (grad_keys, grad_values) = lax.scan(
        step_back, jnp.zeros(queries.shape, jnp.float32), tiles
    )
    return (grad_query, grad_keys, grad_values)


def on_device(
    tokens,
    norm1_gain,
    norm1_bias,
    w_qkv,
    qkv_bias,
    w_out,
    norm2_gain,
    norm2_bias,
    w_gate,
    w_up,
    w_down,
    cotangent,
    seq_lengths,
    block_order,
):
    team_count = lax.axis_size("head")
    span_count = lax.axis_size("blk")
    span_index = lax.axis_index("blk")
    tok_rows = tokens.shape[0]
    model_width = tokens.shape[1]
    group_rows = tok_rows * team_count
    local_width = w_out.shape[0]
    heads_local = local_width // HD
    offsets = jnp.arange(tok_rows, dtype=jnp.int32)
    member = jnp.arange(team_count, dtype=jnp.int32)
    owner_index = jnp.arange(span_count, dtype=jnp.int32)
    query_ids = ((member[:, None] * span_count + span_index) * tok_rows + offsets[None, :]).reshape(
        -1
    )
    key_ids = (
        (member[None, :, None] * span_count + owner_index[:, None, None]) * tok_rows
        + offsets[None, None, :]
    ).reshape(-1)
    query_pos = packed_positions(query_ids, block_order)
    query_start = sequence_start(query_pos, seq_lengths)
    key_pos = packed_positions(key_ids, block_order)
    half_rot = ROT // 2
    freq_table = jnp.power(10000.0, -2.0 * jnp.arange(half_rot, dtype=jnp.float32) / ROT)
    angles = (query_pos - query_start).astype(jnp.float32)[:, None] * freq_table[None, :]
    cosine = jnp.cos(angles)
    sine_table = jnp.sin(angles)
    x_own = tokens.astype(jnp.float32)
    norm1_out, unit_one, inv_one = normalize(x_own, norm1_gain, norm1_bias)
    norm1_group = lax.all_gather(norm1_out.astype(jnp.bfloat16), "head", axis=0, tiled=True)
    qkv_full, out_full = (
        lax.all_gather(w_qkv, "blk", axis=0, tiled=True),
        lax.all_gather(w_out, "blk", axis=1, tiled=True),
    )
    qkv_matrix = qkv_full.reshape(model_width, 3 * local_width)
    projected = jnp.dot(
        norm1_group, qkv_matrix, preferred_element_type=jnp.float32
    ) + qkv_bias.reshape(1, -1)
    projected = projected.reshape(group_rows, 3, heads_local, HD)
    queries = rotate(projected[:, 0], cosine, sine_table).astype(jnp.bfloat16)
    keys_flat = (
        rotate(projected[:, 1], cosine, sine_table)
        .astype(jnp.bfloat16)
        .reshape(group_rows, local_width)
    )
    values_flat = projected[:, 2].astype(jnp.bfloat16).reshape(group_rows, local_width)
    keys_all, values_all = gather_keys(keys_flat, values_flat)
    attn_out, attn_exact, log_norm = attend(
        queries, key_tiles(keys_all, values_all, key_pos, heads_local), query_pos, query_start
    )
    attn_b = attn_out.reshape(group_rows, local_width).astype(jnp.bfloat16)
    attn_own = lax.psum_scatter(
        jnp.dot(attn_b, out_full, preferred_element_type=jnp.float32),
        "head",
        scatter_dimension=0,
        tiled=True,
    )
    hidden = x_own + attn_own
    norm2_out, unit_two, inv_two = normalize(hidden, norm2_gain, norm2_bias)
    norm2_group = lax.all_gather(norm2_out.astype(jnp.bfloat16), "head", axis=0, tiled=True)
    gate_full, up_full, down_full = (
        lax.all_gather(w_gate, "blk", axis=0, tiled=True),
        lax.all_gather(w_up, "blk", axis=0, tiled=True),
        lax.all_gather(w_down, "blk", axis=1, tiled=True),
    )
    gate_val = jnp.dot(norm2_group, gate_full, preferred_element_type=jnp.float32)
    up_val = jnp.dot(norm2_group, up_full, preferred_element_type=jnp.float32)
    sigmoid_gate = jax.nn.sigmoid(gate_val)
    swish_val = gate_val * sigmoid_gate
    activ_b = (swish_val * up_val).astype(jnp.bfloat16)
    mlp_own = lax.psum_scatter(
        jnp.dot(activ_b, down_full, preferred_element_type=jnp.float32).astype(jnp.bfloat16),
        "head",
        scatter_dimension=0,
        tiled=True,
    ).astype(jnp.float32)
    output = (hidden + mlp_own).astype(jnp.bfloat16)
    grad_out = cotangent.astype(jnp.float32)
    grad_group = lax.all_gather(cotangent, "head", axis=0, tiled=True)
    grad_activ = times_transpose(grad_group, down_full)
    grad_w_down = contract_rows(activ_b, grad_group)
    grad_up_b = (grad_activ * swish_val).astype(jnp.bfloat16)
    grad_gate_b = (
        grad_activ * up_val * sigmoid_gate * (1.0 + gate_val * (1.0 - sigmoid_gate))
    ).astype(jnp.bfloat16)
    grad_w_gate = contract_rows(norm2_group, grad_gate_b)
    grad_w_up = contract_rows(norm2_group, grad_up_b)
    grad_norm2 = lax.psum_scatter(
        times_transpose(grad_gate_b, gate_full) + times_transpose(grad_up_b, up_full),
        "head",
        scatter_dimension=0,
        tiled=True,
    )
    grad_hidden = grad_out + normalize_back(grad_norm2, unit_two, inv_two, norm2_gain)
    gain_two_grad = jnp.sum(grad_norm2 * unit_two, axis=0)
    shift_two_grad = jnp.sum(grad_norm2, axis=0)
    branch_group = lax.all_gather(grad_hidden.astype(jnp.bfloat16), "head", axis=0, tiled=True)
    grad_w_out = contract_rows(attn_b, branch_group)
    grad_attn = (
        times_transpose(branch_group, out_full)
        .astype(jnp.bfloat16)
        .reshape(group_rows, heads_local, HD)
    )
    delta_rows = jnp.sum(grad_attn.astype(jnp.float32) * attn_exact, axis=-1).T
    keys_back_all, values_back_all = gather_keys(keys_flat, values_flat)
    tiles_back = key_tiles(keys_back_all, values_back_all, key_pos, heads_local)
    grad_query, grad_keys, grad_values = attend_back(
        queries, tiles_back, query_pos, query_start, log_norm, grad_attn, delta_rows
    )
    key_terms = grad_keys.reshape(-1, local_width)
    value_terms = grad_values.reshape(-1, local_width)
    grad_key_own, grad_value_own = (
        lax.psum_scatter(
            key_terms.astype(jnp.bfloat16), "blk", scatter_dimension=0, tiled=True
        ).astype(jnp.float32),
        lax.psum_scatter(
            value_terms.astype(jnp.bfloat16), "blk", scatter_dimension=0, tiled=True
        ).astype(jnp.float32),
    )
    grad_query_pre = rotate(grad_query, cosine, -sine_table).reshape(group_rows, local_width)
    grad_key_pre = rotate(
        grad_key_own.reshape(group_rows, heads_local, HD), cosine, -sine_table
    ).reshape(group_rows, local_width)
    grad_proj_b = jnp.stack([grad_query_pre, grad_key_pre, grad_value_own], axis=1).astype(
        jnp.bfloat16
    )
    bias_grad = jnp.sum(grad_proj_b.astype(jnp.float32), axis=0)
    grad_proj_flat = grad_proj_b.reshape(group_rows, 3 * local_width)
    grad_w_qkv = contract_rows(norm1_group, grad_proj_flat).reshape(model_width, 3, local_width)
    grad_norm1 = lax.psum_scatter(
        times_transpose(grad_proj_flat, qkv_matrix).astype(jnp.bfloat16),
        "head",
        scatter_dimension=0,
        tiled=True,
    ).astype(jnp.float32)
    input_grad = grad_hidden + normalize_back(grad_norm1, unit_one, inv_one, norm1_gain)
    gain_one_grad = jnp.sum(grad_norm1 * unit_one, axis=0)
    shift_one_grad = jnp.sum(grad_norm1, axis=0)
    norm_sums = (
        lax.psum_scatter(gain_one_grad, ("head", "blk"), scatter_dimension=0, tiled=True),
        lax.psum_scatter(shift_one_grad, ("head", "blk"), scatter_dimension=0, tiled=True),
        lax.psum_scatter(gain_two_grad, ("head", "blk"), scatter_dimension=0, tiled=True),
        lax.psum_scatter(shift_two_grad, ("head", "blk"), scatter_dimension=0, tiled=True),
    )
    grad_shards = (
        lax.psum_scatter(
            grad_w_qkv.astype(jnp.bfloat16), "blk", scatter_dimension=0, tiled=True
        ).astype(jnp.float32),
        lax.psum_scatter(
            bias_grad.astype(jnp.bfloat16), "blk", scatter_dimension=1, tiled=True
        ).astype(jnp.float32),
        lax.psum_scatter(
            grad_w_out.astype(jnp.bfloat16), "blk", scatter_dimension=1, tiled=True
        ).astype(jnp.float32),
        lax.psum_scatter(
            grad_w_gate.astype(jnp.bfloat16), "blk", scatter_dimension=0, tiled=True
        ).astype(jnp.float32),
        lax.psum_scatter(
            grad_w_up.astype(jnp.bfloat16), "blk", scatter_dimension=0, tiled=True
        ).astype(jnp.float32),
        lax.psum_scatter(
            grad_w_down.astype(jnp.bfloat16), "blk", scatter_dimension=1, tiled=True
        ).astype(jnp.float32),
    )
    return (
        output,
        input_grad,
        norm_sums[0],
        norm_sums[1],
        grad_shards[0],
        grad_shards[1],
        grad_shards[2],
        norm_sums[2],
        norm_sums[3],
        grad_shards[3],
        grad_shards[4],
        grad_shards[5],
    )


def split_order(values, z_index, axis):
    pieces = values.shape[axis] // Z_PARTS
    parts = [
        lax.dynamic_slice_in_dim(
            values, lax.rem(z_index - j + Z_PARTS, Z_PARTS) * pieces, pieces, axis
        )
        for j in range(Z_PARTS)
    ]
    return jnp.concatenate(parts, axis=axis)


def swap_x(values):
    return lax.ppermute(values, "head", [(h, h ^ 2) for h in range(4)])


def swap_core(values):
    return lax.ppermute(values, "head", [(h, h ^ 1) for h in range(4)])


def swap_y(values):
    return lax.ppermute(values, "blk", [(b, b ^ 1) for b in range(2 * Z_PARTS)])


def shift_z(values, amount):
    total = 2 * Z_PARTS
    return lax.ppermute(values, "blk", [(b, (b + 2 * amount) % total) for b in range(total)])


def gather_rows(own):
    half = own.shape[0] // 2
    from_x = swap_x(own)
    from_y = swap_y(own)
    corner_a = swap_y(from_x[:half])
    corner_b = swap_x(from_y[half:])
    mine = jnp.concatenate([own, from_y, from_x, corner_a, corner_b], axis=0)
    return jnp.concatenate([mine, swap_core(mine)], axis=0)


def scatter_rows(partial):
    rows = partial.shape[0] // 8
    half = rows // 2
    mine = partial[: 4 * rows]
    theirs = swap_core(partial[4 * rows :].astype(jnp.bfloat16))
    total = mine + theirs.astype(jnp.float32)
    own, for_y, for_x, corner = [total[i * rows : (i + 1) * rows] for i in range(4)]
    corner_b = corner.astype(jnp.bfloat16)
    got_x = swap_x(corner_b[:half]).astype(jnp.float32)
    got_y = swap_y(corner_b[half:]).astype(jnp.float32)
    for_y = jnp.concatenate([for_y[:half] + got_x, for_y[half:]], axis=0)
    for_x = jnp.concatenate([for_x[:half], for_x[half:] + got_y], axis=0)
    last_x = swap_x(for_x.astype(jnp.bfloat16)).astype(jnp.float32)
    last_y = swap_y(for_y.astype(jnp.bfloat16)).astype(jnp.float32)
    return own + last_x + last_y


def ring_gather(chunk, amount):
    held = [chunk]
    for unused in range(Z_PARTS - 1):
        held.append(shift_z(held[-1], amount))
    if amount == 1:
        return held
    return [held[(Z_PARTS - j) % Z_PARTS] for j in range(Z_PARTS)]


def ring_scatter(partials, amount):
    order = [(j + 1) % Z_PARTS for j in range(Z_PARTS)]
    if amount == -1:
        order = [(Z_PARTS - j) % Z_PARTS for j in order]
    total = partials[order[0]]
    for j in order[1:]:
        total = shift_z(total.astype(jnp.bfloat16), amount).astype(jnp.float32) + partials[j]
    return total


def to_even_odd(mine, theirs, y_index):
    got = swap_y(theirs)
    return jnp.where(y_index == 0, mine, got), jnp.where(y_index == 0, got, mine)


def from_even_odd(even, odd, y_index):
    mine = jnp.where(y_index == 0, even, odd)
    theirs = jnp.where(y_index == 0, odd, even).astype(jnp.bfloat16)
    got = swap_y(theirs).astype(jnp.float32)
    return jnp.where(y_index == 0, mine, got), jnp.where(y_index == 0, got, mine)


def to_heads(pieces, z_index):
    received = []
    for t in range(Z_PARTS):
        piece = lax.dynamic_index_in_dim(
            pieces, lax.rem(z_index + t, Z_PARTS), axis=0, keepdims=False
        )
        received.append(piece if t == 0 else shift_z(piece, t))
    return jnp.stack(received, axis=0)


def from_heads(pieces, z_index):
    received = [pieces[0]] + [shift_z(pieces[t], -t) for t in range(1, Z_PARTS)]
    ordered = jnp.stack(received + received, axis=0)
    return lax.dynamic_slice_in_dim(ordered, Z_PARTS - z_index, Z_PARTS, axis=0)


def tile_mask(key_tile, query_tile, start_row):
    key_pos = key_tile * KEY_TILE + lax.broadcasted_iota(jnp.int32, (KEY_TILE, QUERY_TILE), 0)
    query_pos = query_tile * QUERY_TILE + lax.broadcasted_iota(
        jnp.int32, (KEY_TILE, QUERY_TILE), 1
    )
    return (key_pos <= query_pos) & (key_pos >= start_row)


def mm(left, right, left_dim=1, right_dim=0):
    return lax.dot_general(
        left, right, (((left_dim,), (right_dim,)), ((), ())), preferred_element_type=jnp.float32
    )


def pack_blocks(slot_ref, source_ref, target_ref, blocks):
    per_part = source_ref.shape[2] // BLOCK
    for block in range(blocks):
        slot = slot_ref[block]
        part = slot // per_part
        column = pl.multiple_of((slot % per_part) * BLOCK, BLOCK)
        target_ref[:, block * BLOCK : (block + 1) * BLOCK] = source_ref[
            part, :, pl.ds(column, BLOCK)
        ]


def attend_kernel(
    slot_ref, low_ref, qkv_ref, start_ref, out_ref, exact_ref, norm_ref, packed_ref, keys_ref
):
    total = packed_ref.shape[1]
    blocks = total // BLOCK
    pack_blocks(slot_ref, qkv_ref, packed_ref, blocks)
    for tile in range(total // KEY_TILE):
        spot = slice(tile * KEY_TILE, (tile + 1) * KEY_TILE)
        keys_ref[spot, :] = packed_ref[HD : 2 * HD, spot].T

    def query_step(query_tile, unused):
        column = pl.multiple_of(query_tile * QUERY_TILE, QUERY_TILE)
        queries = packed_ref[0:HD, pl.ds(column, QUERY_TILE)] * HD ** (-0.5)
        queries = queries.astype(jnp.bfloat16)
        start_row = start_ref[:, pl.ds(column, QUERY_TILE)]

        def key_step(key_tile, state):
            run_max, run_sum, run_out = state
            row = pl.multiple_of(key_tile * KEY_TILE, KEY_TILE)
            scores = mm(keys_ref[pl.ds(row, KEY_TILE), :], queries)
            scores = jnp.where(tile_mask(key_tile, query_tile, start_row), scores, MASKED)
            new_max = jnp.maximum(run_max, jnp.max(scores, axis=0, keepdims=True))
            probs = jnp.exp(scores - new_max)
            fade = jnp.exp(run_max - new_max)
            run_sum = run_sum * fade + jnp.sum(probs, axis=0, keepdims=True)
            run_out = run_out * fade + mm(
                packed_ref[2 * HD : 3 * HD, pl.ds(row, KEY_TILE)], probs.astype(jnp.bfloat16)
            )
            return new_max, run_sum, run_out

        first = (
            jnp.full((1, QUERY_TILE), -3e38, jnp.float32),
            jnp.zeros((1, QUERY_TILE), jnp.float32),
            jnp.zeros((HD, QUERY_TILE), jnp.float32),
        )
        run_max, run_sum, run_out = lax.fori_loop(
            low_ref[query_tile], ((query_tile + 1) * QUERY_TILE) // KEY_TILE, key_step, first
        )
        exact_ref[:, pl.ds(column, QUERY_TILE)] = run_out / run_sum
        norm_ref[:, pl.ds(column, QUERY_TILE)] = run_max + jnp.log(run_sum)
        return unused

    lax.fori_loop(0, total // QUERY_TILE, query_step, 0)
    per_part = out_ref.shape[2] // BLOCK
    for block in range(blocks):
        slot = slot_ref[block]
        column = pl.multiple_of((slot % per_part) * BLOCK, BLOCK)
        out_ref[slot // per_part, :, pl.ds(column, BLOCK)] = exact_ref[
            :, block * BLOCK : (block + 1) * BLOCK
        ].astype(jnp.bfloat16)


def rotate_back(values, cosine, sine_table):
    half_rot = ROT // 2
    lead_part = values[0:half_rot]
    tail_part = values[half_rot:ROT]
    return jnp.concatenate(
        [
            lead_part * cosine + tail_part * sine_table,
            tail_part * cosine - lead_part * sine_table,
            values[ROT:],
        ],
        axis=0,
    )


def attend_back_kernel(
    slot_ref,
    low_ref,
    grad_ref,
    packed_ref,
    exact_ref,
    norm_ref,
    start_ref,
    cosine_ref,
    sine_ref,
    out_ref,
    bias_ref,
    keys_ref,
    values_ref,
    grads_ref,
    sums_ref,
):
    total = packed_ref.shape[1]
    blocks = total // BLOCK
    scale = HD ** (-0.5)
    pack_blocks(slot_ref, grad_ref, grads_ref, blocks)
    for tile in range(total // KEY_TILE):
        spot = slice(tile * KEY_TILE, (tile + 1) * KEY_TILE)
        keys_ref[spot, :] = packed_ref[HD : 2 * HD, spot].T
        values_ref[spot, :] = packed_ref[2 * HD : 3 * HD, spot].T
    sums_ref[HD : 3 * HD, :] = jnp.zeros((2 * HD, total), jnp.float32)

    def query_step(query_tile, unused):
        column = pl.multiple_of(query_tile * QUERY_TILE, QUERY_TILE)
        spot = pl.ds(column, QUERY_TILE)
        queries = (packed_ref[0:HD, spot] * scale).astype(jnp.bfloat16)
        grads = grads_ref[:, spot]
        start_row = start_ref[:, spot]
        norm_row = norm_ref[:, spot]
        delta_row = jnp.sum(
            grads.astype(jnp.float32) * exact_ref[:, spot], axis=0, keepdims=True
        )

        def key_step(key_tile, grad_query):
            row = pl.multiple_of(key_tile * KEY_TILE, KEY_TILE)
            rows = pl.ds(row, KEY_TILE)
            scores = mm(keys_ref[rows, :], queries)
            scores = jnp.where(tile_mask(key_tile, query_tile, start_row), scores, MASKED)
            probs = jnp.exp(scores - norm_row)
            grad_probs = mm(values_ref[rows, :], grads)
            grad_scores = (probs * (grad_probs - delta_row)).astype(jnp.bfloat16)
            probs_b = probs.astype(jnp.bfloat16)
            sums_ref[2 * HD : 3 * HD, rows] += mm(grads, probs_b, 1, 1)
            sums_ref[HD : 2 * HD, rows] += mm(queries, grad_scores, 1, 1)
            return grad_query + mm(packed_ref[HD : 2 * HD, rows], grad_scores)

        grad_query = lax.fori_loop(
            low_ref[query_tile],
            ((query_tile + 1) * QUERY_TILE) // KEY_TILE,
            key_step,
            jnp.zeros((HD, QUERY_TILE), jnp.float32),
        )
        sums_ref[0:HD, spot] = grad_query * scale
        return unused

    lax.fori_loop(0, total // QUERY_TILE, query_step, 0)
    per_part = out_ref.shape[2] // BLOCK
    bias_sum = jnp.zeros((3 * HD, BLOCK), jnp.float32)
    for block in range(blocks):
        spot = slice(block * BLOCK, (block + 1) * BLOCK)
        cosine = cosine_ref[:, spot]
        sine_table = sine_ref[:, spot]
        slot = slot_ref[block]
        column = pl.multiple_of((slot % per_part) * BLOCK, BLOCK)
        rounded = jnp.concatenate(
            [
                rotate_back(sums_ref[0:HD, spot], cosine, sine_table),
                rotate_back(sums_ref[HD : 2 * HD, spot], cosine, sine_table),
                sums_ref[2 * HD : 3 * HD, spot],
            ],
            axis=0,
        ).astype(jnp.bfloat16)
        out_ref[slot // per_part, :, pl.ds(column, BLOCK)] = rounded
        bias_sum = bias_sum + rounded.astype(jnp.float32)
    bias_ref[...] = bias_sum


def attend_heads(slot_of, low_tile, qkv_parts, start_row):
    parts, features, part_rows = qkv_parts.shape
    total = parts * part_rows
    vmem = pl.BlockSpec(memory_space=pltpu.VMEM)
    return pl.pallas_call(
        attend_kernel,
        grid_spec=pltpu.PrefetchScalarGridSpec(
            num_scalar_prefetch=2,
            grid=(1,),
            in_specs=[vmem, vmem],
            out_specs=[vmem, vmem, vmem, vmem],
            scratch_shapes=[pltpu.VMEM((total, HD), jnp.bfloat16)],
        ),
        out_shape=[
            jax.ShapeDtypeStruct((parts, HD, part_rows), jnp.bfloat16),
            jax.ShapeDtypeStruct((HD, total), jnp.float32),
            jax.ShapeDtypeStruct((1, total), jnp.float32),
            jax.ShapeDtypeStruct((3 * HD, total), jnp.bfloat16),
        ],
        cost_estimate=pl.CostEstimate(
            flops=total * total * HD, transcendentals=total * total // 4, bytes_accessed=6 << 20
        ),
        compiler_params=pltpu.CompilerParams(vmem_limit_bytes=40 << 20),
        name="attend",
    )(slot_of, low_tile, qkv_parts, start_row)


def attend_heads_back(
    slot_of, low_tile, grad_parts, packed, exact, log_norm, start_row, cosine, sine_table
):
    parts, features, part_rows = grad_parts.shape
    total = parts * part_rows
    vmem = pl.BlockSpec(memory_space=pltpu.VMEM)
    return pl.pallas_call(
        attend_back_kernel,
        grid_spec=pltpu.PrefetchScalarGridSpec(
            num_scalar_prefetch=2,
            grid=(1,),
            in_specs=[vmem] * 7,
            out_specs=[vmem, vmem],
            scratch_shapes=[
                pltpu.VMEM((total, HD), jnp.bfloat16),
                pltpu.VMEM((total, HD), jnp.bfloat16),
                pltpu.VMEM((HD, total), jnp.bfloat16),
                pltpu.VMEM((3 * HD, total), jnp.float32),
            ],
        ),
        out_shape=[
            jax.ShapeDtypeStruct((parts, 3 * HD, part_rows), jnp.bfloat16),
            jax.ShapeDtypeStruct((3 * HD, BLOCK), jnp.float32),
        ],
        cost_estimate=pl.CostEstimate(
            flops=3 * total * total * HD,
            transcendentals=total * total // 4,
            bytes_accessed=8 << 20,
        ),
        compiler_params=pltpu.CompilerParams(vmem_limit_bytes=50 << 20),
        name="attend_back",
    )(slot_of, low_tile, grad_parts, packed, exact, log_norm, start_row, cosine, sine_table)


def start_of(position, seq_lengths):
    seq_ends = jnp.cumsum(seq_lengths)
    ends_before = seq_ends[:, None] <= position[None, :]
    return jnp.sum(jnp.where(ends_before, seq_lengths[:, None], 0), axis=0)


def rotary_tables(offset_in_seq):
    half_rot = ROT // 2
    freq_table = jnp.power(10000.0, -2.0 * jnp.arange(half_rot, dtype=jnp.float32) / ROT)
    angles = freq_table[:, None] * offset_in_seq.astype(jnp.float32)[None, :]
    return jnp.cos(angles), jnp.sin(angles)


def on_device_heads(
    tokens,
    norm1_gain,
    norm1_bias,
    w_qkv,
    qkv_bias,
    w_out,
    norm2_gain,
    norm2_bias,
    w_gate,
    w_up,
    w_down,
    cotangent,
    seq_lengths,
    block_order,
):
    head_index = lax.axis_index("head")
    blk_index = lax.axis_index("blk")
    x_index, core_index = head_index // 2, head_index % 2
    z_index, y_index = blk_index // 2, blk_index % 2
    tok_rows, model_width = tokens.shape
    plane_rows = 8 * tok_rows
    total_rows = Z_PARTS * plane_rows
    row_block = model_width // (2 * Z_PARTS)
    chunk = 2 * row_block
    ff_half = w_gate.shape[1] // 2
    heads_width = Z_PARTS * HD

    qkv_split = w_qkv.reshape(row_block, 3, Z_PARTS, 2, HD)
    qkv_low = qkv_split[:, :, :, 0].reshape(row_block, 3 * heads_width)
    qkv_high = qkv_split[:, :, :, 1].reshape(row_block, 3 * heads_width)
    first = y_index == 0
    qkv_even, qkv_odd = to_even_odd(
        jnp.where(first, qkv_low, qkv_high), jnp.where(first, qkv_high, qkv_low), y_index
    )
    out_split = w_out.reshape(Z_PARTS, 2, HD, row_block)
    out_low = out_split[:, 0].reshape(heads_width, row_block)
    out_high = out_split[:, 1].reshape(heads_width, row_block)
    out_even, out_odd = to_even_odd(
        jnp.where(first, out_low, out_high), jnp.where(first, out_high, out_low), y_index
    )

    def column_halves(weight):
        low, high = weight[:, :ff_half], weight[:, ff_half:]
        return to_even_odd(jnp.where(first, low, high), jnp.where(first, high, low), y_index)

    gate_own = jnp.concatenate(column_halves(w_gate), axis=0)
    up_own = jnp.concatenate(column_halves(w_up), axis=0)
    down_low, down_high = w_down[:ff_half], w_down[ff_half:]
    down_even, down_odd = to_even_odd(
        jnp.where(first, down_low, down_high), jnp.where(first, down_high, down_low), y_index
    )

    def both_ways(even, odd, axis):
        forward = ring_gather(even, 1)
        backward = ring_gather(odd, -1)
        pieces = [p for pair in zip(forward, backward) for p in pair]
        return jnp.concatenate(pieces, axis=axis)

    x_own = split_order(tokens, z_index, 1).astype(jnp.float32)
    gain_one = split_order(norm1_gain, z_index, 0)
    shift_one = split_order(norm1_bias, z_index, 0)
    gain_two = split_order(norm2_gain, z_index, 0)
    shift_two = split_order(norm2_bias, z_index, 0)
    norm1_out, unit_one, inv_one = normalize(x_own, gain_one, shift_one)
    norm1_all = gather_rows(norm1_out.astype(jnp.bfloat16))
    qkv_full = both_ways(qkv_even, qkv_odd, 0)
    out_full = both_ways(out_even, out_odd, 1)
    gate_full = jnp.concatenate(ring_gather(gate_own, 1), axis=0)
    up_full = jnp.concatenate(ring_gather(up_own, -1), axis=0)
    down_full = both_ways(down_even, down_odd, 1)

    slots = jnp.arange(Z_PARTS * 8, dtype=jnp.int32)
    step_z, flip = slots // 8, slots % 8
    owner = (
        ((x_index ^ ((flip // 2) % 2)) * 2 + (core_index ^ (flip // 4))) * (2 * Z_PARTS)
        + ((z_index - step_z + Z_PARTS) % Z_PARTS) * 2
        + (y_index ^ (flip % 2))
    )
    packed_block = jnp.sum(
        jnp.where(owner[:, None] == slots[None, :], block_order[None, :], 0), axis=1
    )
    slot_of = jnp.sum(
        jnp.where(packed_block[None, :] == slots[:, None], slots[None, :], 0), axis=1
    )
    plane_pos = (
        packed_block[:8, None] * BLOCK + jnp.arange(BLOCK, dtype=jnp.int32)[None, :]
    ).reshape(-1)
    plane_cos, plane_sin = rotary_tables(plane_pos - start_of(plane_pos, seq_lengths))
    all_pos = jnp.arange(total_rows, dtype=jnp.int32)
    all_start = start_of(all_pos, seq_lengths)
    all_cos, all_sin = rotary_tables(all_pos - all_start)
    low_tile = (
        start_of(
            jnp.arange(total_rows // QUERY_TILE, dtype=jnp.int32) * QUERY_TILE, seq_lengths
        )
        // KEY_TILE
    )
    start_row = all_start[None, :]

    bias_split = qkv_bias.reshape(3, Z_PARTS, 2, HD)
    bias_own = jnp.where(first, bias_split[:, :, 0], bias_split[:, :, 1]).reshape(-1)
    projected = (mm(qkv_full, norm1_all, 0, 1) + bias_own[:, None]).reshape(
        3, Z_PARTS, HD, plane_rows
    )
    half_rot = ROT // 2
    lead_part, tail_part = projected[:2, :, :half_rot], projected[:2, :, half_rot:ROT]
    rotated = jnp.concatenate(
        [
            lead_part * plane_cos - tail_part * plane_sin,
            tail_part * plane_cos + lead_part * plane_sin,
            projected[:2, :, ROT:],
        ],
        axis=2,
    )
    qkv_heads = jnp.concatenate([rotated, projected[2:]], axis=0).astype(jnp.bfloat16)
    qkv_heads = qkv_heads.transpose(1, 0, 2, 3).reshape(Z_PARTS, 3 * HD, plane_rows)
    qkv_parts = to_heads(qkv_heads, z_index)
    attn_parts, attn_exact, log_norm, packed = attend_heads(
        slot_of, low_tile, qkv_parts, start_row
    )
    attn_t = from_heads(attn_parts, z_index).reshape(heads_width, plane_rows)
    attn_own = scatter_rows(mm(attn_t, out_full, 0, 0))

    hidden = x_own + attn_own
    norm2_out, unit_two, inv_two = normalize(hidden, gain_two, shift_two)
    norm2_all = gather_rows(norm2_out.astype(jnp.bfloat16))
    cotangent_own = split_order(cotangent, z_index, 1)
    grad_all = gather_rows(cotangent_own)
    gate_val = mm(norm2_all, gate_full)
    up_val = mm(norm2_all, up_full)
    sigmoid_gate = jax.nn.sigmoid(gate_val)
    swish_val = gate_val * sigmoid_gate
    activ_b = (swish_val * up_val).astype(jnp.bfloat16)
    grad_activ = mm(grad_all, down_full, 1, 1)
    grad_up_b = (grad_activ * swish_val).astype(jnp.bfloat16)
    grad_gate_b = (
        grad_activ * up_val * sigmoid_gate * (1.0 + gate_val * (1.0 - sigmoid_gate))
    ).astype(jnp.bfloat16)
    grad_norm2 = scatter_rows(mm(grad_gate_b, gate_full, 1, 1) + mm(grad_up_b, up_full, 1, 1))
    mlp_own = scatter_rows(mm(activ_b, down_full))
    output = split_order((hidden + mlp_own).astype(jnp.bfloat16), z_index, 1)

    def pieces_of(values, width, offset=0, size=None):
        size = width if size is None else size
        return [
            values[:, j * width + offset : j * width + offset + size] for j in range(Z_PARTS)
        ]

    down_sum_even = ring_scatter(
        [mm(activ_b, p, 0, 0) for p in pieces_of(grad_all, chunk, 0, row_block)], 1
    )
    down_sum_odd = ring_scatter(
        [mm(activ_b, p, 0, 0) for p in pieces_of(grad_all, chunk, row_block, row_block)], -1
    )
    down_parts = from_even_odd(down_sum_even, down_sum_odd, y_index)
    down_grad = jnp.concatenate(down_parts, axis=0)
    gate_sum = ring_scatter([mm(p, grad_gate_b, 0, 0) for p in pieces_of(norm2_all, chunk)], 1)
    up_sum = ring_scatter([mm(p, grad_up_b, 0, 0) for p in pieces_of(norm2_all, chunk)], -1)
    gate_grad = jnp.concatenate(
        from_even_odd(gate_sum[:row_block], gate_sum[row_block:], y_index), axis=1
    )
    up_grad = jnp.concatenate(
        from_even_odd(up_sum[:row_block], up_sum[row_block:], y_index), axis=1
    )

    grad_out = cotangent_own.astype(jnp.float32)
    grad_hidden = grad_out + normalize_back(grad_norm2, unit_two, inv_two, gain_two)
    branch_all = gather_rows(grad_hidden.astype(jnp.bfloat16))
    grad_attn = (
        mm(out_full, branch_all, 1, 1)
        .astype(jnp.bfloat16)
        .reshape(Z_PARTS, HD, plane_rows)
    )
    grad_parts = to_heads(grad_attn, z_index)
    proj_parts, bias_sums = attend_heads_back(
        slot_of, low_tile, grad_parts, packed, attn_exact, log_norm, start_row, all_cos, all_sin
    )
    bias_grad = jnp.sum(bias_sums, axis=1).reshape(3, HD)
    grad_proj = from_heads(proj_parts, z_index).reshape(Z_PARTS, 3, HD, plane_rows)
    grad_proj = grad_proj.transpose(1, 0, 2, 3).reshape(3 * heads_width, plane_rows)
    grad_norm1 = scatter_rows(mm(grad_proj, qkv_full, 0, 1))

    out_sum_even = ring_scatter(
        [mm(attn_t, p) for p in pieces_of(branch_all, chunk, 0, row_block)], 1
    )
    out_sum_odd = ring_scatter(
        [mm(attn_t, p) for p in pieces_of(branch_all, chunk, row_block, row_block)], -1
    )
    out_parts = from_even_odd(out_sum_even, out_sum_odd, y_index)
    out_grad = jnp.stack(
        [p.reshape(Z_PARTS, HD, row_block) for p in out_parts], axis=1
    ).reshape(w_out.shape)
    qkv_sum_even = ring_scatter(
        [mm(p, grad_proj, 0, 1) for p in pieces_of(norm1_all, chunk, 0, row_block)], 1
    )
    qkv_sum_odd = ring_scatter(
        [mm(p, grad_proj, 0, 1) for p in pieces_of(norm1_all, chunk, row_block, row_block)], -1
    )
    qkv_grad_parts = from_even_odd(qkv_sum_even, qkv_sum_odd, y_index)
    qkv_grad = jnp.stack(
        [p.reshape(row_block, 3, Z_PARTS, HD) for p in qkv_grad_parts], axis=3
    ).reshape(w_qkv.shape)

    input_grad = grad_hidden + normalize_back(grad_norm1, unit_one, inv_one, gain_one)
    sums = jnp.stack(
        [
            jnp.sum(grad_norm1 * unit_one, axis=0),
            jnp.sum(grad_norm1, axis=0),
            jnp.sum(grad_norm2 * unit_two, axis=0),
            jnp.sum(grad_norm2, axis=0),
        ],
        axis=0,
    )
    norm_sums = lax.psum_scatter(
        split_order(sums, z_index, 1), ("head", "blk"), scatter_dimension=1, tiled=True
    )
    return (
        output,
        split_order(input_grad, z_index, 1),
        norm_sums[0],
        norm_sums[1],
        qkv_grad,
        bias_grad,
        out_grad,
        norm_sums[2],
        norm_sums[3],
        gate_grad,
        up_grad,
        down_grad,
    )


def solution(mesh):
    placed = (
        P(("head", "blk"), None),
        P(),
        P(),
        P("blk", None, "head"),
        P(None, "head"),
        P("head", "blk"),
        P(),
        P(),
        P("blk", "head"),
        P("blk", "head"),
        P("head", "blk"),
        P(("head", "blk"), None),
        P(),
        P(),
    )
    heads_plan = mesh.shape["head"] == 4 and mesh.shape["blk"] == 2 * Z_PARTS
    return jax.shard_map(
        on_device_heads if heads_plan else on_device,
        mesh=mesh,
        in_specs=placed,
        out_specs=(
            P(("head", "blk"), None),
            P(("head", "blk"), None),
            P(("head", "blk")),
            P(("head", "blk")),
            P("blk", None, "head"),
            P(None, ("head", "blk")),
            P("head", "blk"),
            P(("head", "blk")),
            P(("head", "blk")),
            P("blk", "head"),
            P("blk", "head"),
            P("head", "blk"),
        ),
        check_vma=False,
    )
```

```python
import jax
import jax.numpy as jnp
from jax import lax
from jax.experimental import pallas as pl
from jax.experimental.pallas import tpu as pltpu
from jax.sharding import PartitionSpec as P

HD = 64
ROT = 16
BLOCK = 128
Z_PARTS = 4
QUERY_TILE = 512
KEY_TILE = 256


EPSILON = 1e-05
MASKED = -1000000000.0


def contract_rows(left, right):
    return lax.dot_general(
        left, right, (((0,), (0,)), ((), ())), preferred_element_type=jnp.float32
    )


def times_transpose(left, right):
    return lax.dot_general(
        left, right, (((1,), (1,)), ((), ())), preferred_element_type=jnp.float32
    )


def packed_positions(row_ids, block_order):
    block_ids = jnp.arange(block_order.shape[0], dtype=jnp.int32)
    matches = (row_ids // BLOCK)[:, None] == block_ids[None, :]
    block_start = jnp.sum(jnp.where(matches, block_order[None, :], 0), axis=1)
    return block_start * BLOCK + row_ids % BLOCK


def sequence_start(position, seq_lengths):
    seq_ends = jnp.cumsum(seq_lengths)
    ends_before = seq_ends[None, :] <= position[:, None]
    return jnp.sum(jnp.where(ends_before, seq_lengths[None, :], 0), axis=1)


def rotate(values, cosine, sine_table):
    half_rot = ROT // 2
    lead_part = values[..., :half_rot]
    tail_part = values[..., half_rot:ROT]
    cos_rows = cosine[:, None, :]
    sin_rows = sine_table[:, None, :]
    return jnp.concatenate(
        [
            lead_part * cos_rows - tail_part * sin_rows,
            tail_part * cos_rows + lead_part * sin_rows,
            values[..., ROT:],
        ],
        axis=-1,
    )


def normalize(values, norm_gain, norm_shift):
    centre = values - jnp.mean(values, axis=-1, keepdims=True)
    inv_scale = lax.rsqrt(jnp.mean(centre * centre, axis=-1, keepdims=True) + EPSILON)
    unit_rows = centre * inv_scale
    return (unit_rows * norm_gain + norm_shift, unit_rows, inv_scale)


def normalize_back(grad_norm, unit_rows, inv_scale, norm_gain):
    grad_unit = grad_norm * norm_gain
    mean_grad = jnp.mean(grad_unit, axis=-1, keepdims=True)
    mean_proj = jnp.mean(grad_unit * unit_rows, axis=-1, keepdims=True)
    return inv_scale * (grad_unit - mean_grad - unit_rows * mean_proj)


def gather_keys(keys_flat, values_flat):
    return (
        lax.all_gather(keys_flat, "blk", axis=0, tiled=True),
        lax.all_gather(values_flat, "blk", axis=0, tiled=True),
    )


def tile_count_of(total_rows):
    tile_rows = min(1024, total_rows)
    return (total_rows // tile_rows, tile_rows)


def key_tiles(keys_all, values_all, key_pos, heads_local):
    tile_count, tile_rows = tile_count_of(keys_all.shape[0])
    return (
        keys_all.reshape(tile_count, tile_rows, heads_local, HD),
        values_all.reshape(tile_count, tile_rows, heads_local, HD),
        key_pos.reshape(tile_count, tile_rows),
    )


def masked_scores(queries, key_tile, pos_tile, query_pos, query_start):
    raw_scores = jnp.einsum(
        "qhd,khd->hqk", queries, key_tile, preferred_element_type=jnp.float32
    ) * HD ** (-0.5)
    allowed = (pos_tile[None, :] <= query_pos[:, None]) & (
        pos_tile[None, :] >= query_start[:, None]
    )
    return jnp.where(allowed[None], raw_scores, MASKED)


def attend(queries, tiles, query_pos, query_start):
    group_rows = queries.shape[0]
    heads_local = queries.shape[1]

    def first_pass(run_state, tile):
        run_max, run_sum = run_state
        scores = masked_scores(queries, tile[0], tile[2], query_pos, query_start)
        new_max = jnp.maximum(run_max, jnp.max(scores, axis=-1))
        new_sum = run_sum * jnp.exp(run_max - new_max) + jnp.sum(
            jnp.exp(scores - new_max[..., None]), axis=-1
        )
        return ((new_max, new_sum), None)

    start_state = (
        jnp.full((heads_local, group_rows), -3e38, jnp.float32),
        jnp.zeros((heads_local, group_rows), jnp.float32),
    )
    (run_max, run_sum), unused = lax.scan(first_pass, start_state, tiles)
    log_norm = run_max + jnp.log(run_sum)

    def second_pass(totals, tile):
        total_out, total_rest = totals
        scores = masked_scores(queries, tile[0], tile[2], query_pos, query_start)
        probs_f32 = jnp.exp(scores - log_norm[..., None])
        probs_b = probs_f32.astype(jnp.bfloat16)
        rest_b = (probs_f32 - probs_b.astype(jnp.float32)).astype(jnp.bfloat16)
        total_out = total_out + jnp.einsum(
            "hqk,khd->qhd", probs_b, tile[1], preferred_element_type=jnp.float32
        )
        total_rest = total_rest + jnp.einsum(
            "hqk,khd->qhd", rest_b, tile[1], preferred_element_type=jnp.float32
        )
        return ((total_out, total_rest), None)

    empty = jnp.zeros((group_rows, heads_local, HD), jnp.float32)
    (attended, leftover), unused = lax.scan(second_pass, (empty, empty), tiles)
    return (attended, attended + leftover, log_norm)


def attend_back(queries, tiles, query_pos, query_start, log_norm, grad_attn, delta_rows):
    scale = HD ** (-0.5)

    def step_back(grad_query, tile):
        key_tile, value_tile, pos_tile = tile
        scores = masked_scores(queries, key_tile, pos_tile, query_pos, query_start)
        probs_f32 = jnp.exp(scores - log_norm[..., None])
        grad_probs = jnp.einsum(
            "qhd,khd->hqk", grad_attn, value_tile, preferred_element_type=jnp.float32
        )
        grad_scores = (probs_f32 * (grad_probs - delta_rows[..., None])).astype(jnp.bfloat16)
        probs_b = probs_f32.astype(jnp.bfloat16)
        grad_query = grad_query + scale * jnp.einsum(
            "hqk,khd->qhd", grad_scores, key_tile, preferred_element_type=jnp.float32
        )
        grad_key = scale * jnp.einsum(
            "hqk,qhd->khd", grad_scores, queries, preferred_element_type=jnp.float32
        )
        grad_value = jnp.einsum(
            "hqk,qhd->khd", probs_b, grad_attn, preferred_element_type=jnp.float32
        )
        return (grad_query, (grad_key, grad_value))

    grad_query, (grad_keys, grad_values) = lax.scan(
        step_back, jnp.zeros(queries.shape, jnp.float32), tiles
    )
    return (grad_query, grad_keys, grad_values)


def on_device(
    tokens,
    norm1_gain,
    norm1_bias,
    w_qkv,
    qkv_bias,
    w_out,
    norm2_gain,
    norm2_bias,
    w_gate,
    w_up,
    w_down,
    cotangent,
    seq_lengths,
    block_order,
):
    team_count = lax.axis_size("head")
    span_count = lax.axis_size("blk")
    span_index = lax.axis_index("blk")
    tok_rows = tokens.shape[0]
    model_width = tokens.shape[1]
    group_rows = tok_rows * team_count
    local_width = w_out.shape[0]
    heads_local = local_width // HD
    offsets = jnp.arange(tok_rows, dtype=jnp.int32)
    member = jnp.arange(team_count, dtype=jnp.int32)
    owner_index = jnp.arange(span_count, dtype=jnp.int32)
    query_ids = ((member[:, None] * span_count + span_index) * tok_rows + offsets[None, :]).reshape(
        -1
    )
    key_ids = (
        (member[None, :, None] * span_count + owner_index[:, None, None]) * tok_rows
        + offsets[None, None, :]
    ).reshape(-1)
    query_pos = packed_positions(query_ids, block_order)
    query_start = sequence_start(query_pos, seq_lengths)
    key_pos = packed_positions(key_ids, block_order)
    half_rot = ROT // 2
    freq_table = jnp.power(10000.0, -2.0 * jnp.arange(half_rot, dtype=jnp.float32) / ROT)
    angles = (query_pos - query_start).astype(jnp.float32)[:, None] * freq_table[None, :]
    cosine = jnp.cos(angles)
    sine_table = jnp.sin(angles)
    x_own = tokens.astype(jnp.float32)
    norm1_out, unit_one, inv_one = normalize(x_own, norm1_gain, norm1_bias)
    norm1_group = lax.all_gather(norm1_out.astype(jnp.bfloat16), "head", axis=0, tiled=True)
    qkv_full, out_full = (
        lax.all_gather(w_qkv, "blk", axis=0, tiled=True),
        lax.all_gather(w_out, "blk", axis=1, tiled=True),
    )
    qkv_matrix = qkv_full.reshape(model_width, 3 * local_width)
    projected = jnp.dot(
        norm1_group, qkv_matrix, preferred_element_type=jnp.float32
    ) + qkv_bias.reshape(1, -1)
    projected = projected.reshape(group_rows, 3, heads_local, HD)
    queries = rotate(projected[:, 0], cosine, sine_table).astype(jnp.bfloat16)
    keys_flat = (
        rotate(projected[:, 1], cosine, sine_table)
        .astype(jnp.bfloat16)
        .reshape(group_rows, local_width)
    )
    values_flat = projected[:, 2].astype(jnp.bfloat16).reshape(group_rows, local_width)
    keys_all, values_all = gather_keys(keys_flat, values_flat)
    attn_out, attn_exact, log_norm = attend(
        queries, key_tiles(keys_all, values_all, key_pos, heads_local), query_pos, query_start
    )
    attn_b = attn_out.reshape(group_rows, local_width).astype(jnp.bfloat16)
    attn_own = lax.psum_scatter(
        jnp.dot(attn_b, out_full, preferred_element_type=jnp.float32),
        "head",
        scatter_dimension=0,
        tiled=True,
    )
    hidden = x_own + attn_own
    norm2_out, unit_two, inv_two = normalize(hidden, norm2_gain, norm2_bias)
    norm2_group = lax.all_gather(norm2_out.astype(jnp.bfloat16), "head", axis=0, tiled=True)
    gate_full, up_full, down_full = (
        lax.all_gather(w_gate, "blk", axis=0, tiled=True),
        lax.all_gather(w_up, "blk", axis=0, tiled=True),
        lax.all_gather(w_down, "blk", axis=1, tiled=True),
    )
    gate_val = jnp.dot(norm2_group, gate_full, preferred_element_type=jnp.float32)
    up_val = jnp.dot(norm2_group, up_full, preferred_element_type=jnp.float32)
    sigmoid_gate = jax.nn.sigmoid(gate_val)
    swish_val = gate_val * sigmoid_gate
    activ_b = (swish_val * up_val).astype(jnp.bfloat16)
    mlp_own = lax.psum_scatter(
        jnp.dot(activ_b, down_full, preferred_element_type=jnp.float32).astype(jnp.bfloat16),
        "head",
        scatter_dimension=0,
        tiled=True,
    ).astype(jnp.float32)
    output = (hidden + mlp_own).astype(jnp.bfloat16)
    grad_out = cotangent.astype(jnp.float32)
    grad_group = lax.all_gather(cotangent, "head", axis=0, tiled=True)
    grad_activ = times_transpose(grad_group, down_full)
    grad_w_down = contract_rows(activ_b, grad_group)
    grad_up_b = (grad_activ * swish_val).astype(jnp.bfloat16)
    grad_gate_b = (
        grad_activ * up_val * sigmoid_gate * (1.0 + gate_val * (1.0 - sigmoid_gate))
    ).astype(jnp.bfloat16)
    grad_w_gate = contract_rows(norm2_group, grad_gate_b)
    grad_w_up = contract_rows(norm2_group, grad_up_b)
    grad_norm2 = lax.psum_scatter(
        times_transpose(grad_gate_b, gate_full) + times_transpose(grad_up_b, up_full),
        "head",
        scatter_dimension=0,
        tiled=True,
    )
    grad_hidden = grad_out + normalize_back(grad_norm2, unit_two, inv_two, norm2_gain)
    gain_two_grad = jnp.sum(grad_norm2 * unit_two, axis=0)
    shift_two_grad = jnp.sum(grad_norm2, axis=0)
    branch_group = lax.all_gather(grad_hidden.astype(jnp.bfloat16), "head", axis=0, tiled=True)
    grad_w_out = contract_rows(attn_b, branch_group)
    grad_attn = (
        times_transpose(branch_group, out_full)
        .astype(jnp.bfloat16)
        .reshape(group_rows, heads_local, HD)
    )
    delta_rows = jnp.sum(grad_attn.astype(jnp.float32) * attn_exact, axis=-1).T
    keys_back_all, values_back_all = gather_keys(keys_flat, values_flat)
    tiles_back = key_tiles(keys_back_all, values_back_all, key_pos, heads_local)
    grad_query, grad_keys, grad_values = attend_back(
        queries, tiles_back, query_pos, query_start, log_norm, grad_attn, delta_rows
    )
    key_terms = grad_keys.reshape(-1, local_width)
    value_terms = grad_values.reshape(-1, local_width)
    grad_key_own, grad_value_own = (
        lax.psum_scatter(
            key_terms.astype(jnp.bfloat16), "blk", scatter_dimension=0, tiled=True
        ).astype(jnp.float32),
        lax.psum_scatter(
            value_terms.astype(jnp.bfloat16), "blk", scatter_dimension=0, tiled=True
        ).astype(jnp.float32),
    )
    grad_query_pre = rotate(grad_query, cosine, -sine_table).reshape(group_rows, local_width)
    grad_key_pre = rotate(
        grad_key_own.reshape(group_rows, heads_local, HD), cosine, -sine_table
    ).reshape(group_rows, local_width)
    grad_proj_b = jnp.stack([grad_query_pre, grad_key_pre, grad_value_own], axis=1).astype(
        jnp.bfloat16
    )
    bias_grad = jnp.sum(grad_proj_b.astype(jnp.float32), axis=0)
    grad_proj_flat = grad_proj_b.reshape(group_rows, 3 * local_width)
    grad_w_qkv = contract_rows(norm1_group, grad_proj_flat).reshape(model_width, 3, local_width)
    grad_norm1 = lax.psum_scatter(
        times_transpose(grad_proj_flat, qkv_matrix).astype(jnp.bfloat16),
        "head",
        scatter_dimension=0,
        tiled=True,
    ).astype(jnp.float32)
    input_grad = grad_hidden + normalize_back(grad_norm1, unit_one, inv_one, norm1_gain)
    gain_one_grad = jnp.sum(grad_norm1 * unit_one, axis=0)
    shift_one_grad = jnp.sum(grad_norm1, axis=0)
    norm_sums = (
        lax.psum_scatter(gain_one_grad, ("head", "blk"), scatter_dimension=0, tiled=True),
        lax.psum_scatter(shift_one_grad, ("head", "blk"), scatter_dimension=0, tiled=True),
        lax.psum_scatter(gain_two_grad, ("head", "blk"), scatter_dimension=0, tiled=True),
        lax.psum_scatter(shift_two_grad, ("head", "blk"), scatter_dimension=0, tiled=True),
    )
    grad_shards = (
        lax.psum_scatter(
            grad_w_qkv.astype(jnp.bfloat16), "blk", scatter_dimension=0, tiled=True
        ).astype(jnp.float32),
        lax.psum_scatter(
            bias_grad.astype(jnp.bfloat16), "blk", scatter_dimension=1, tiled=True
        ).astype(jnp.float32),
        lax.psum_scatter(
            grad_w_out.astype(jnp.bfloat16), "blk", scatter_dimension=1, tiled=True
        ).astype(jnp.float32),
        lax.psum_scatter(
            grad_w_gate.astype(jnp.bfloat16), "blk", scatter_dimension=0, tiled=True
        ).astype(jnp.float32),
        lax.psum_scatter(
            grad_w_up.astype(jnp.bfloat16), "blk", scatter_dimension=0, tiled=True
        ).astype(jnp.float32),
        lax.psum_scatter(
            grad_w_down.astype(jnp.bfloat16), "blk", scatter_dimension=1, tiled=True
        ).astype(jnp.float32),
    )
    return (
        output,
        input_grad,
        norm_sums[0],
        norm_sums[1],
        grad_shards[0],
        grad_shards[1],
        grad_shards[2],
        norm_sums[2],
        norm_sums[3],
        grad_shards[3],
        grad_shards[4],
        grad_shards[5],
    )


def split_order(values, z_index, axis):
    pieces = values.shape[axis] // Z_PARTS
    parts = [
        lax.dynamic_slice_in_dim(
            values, lax.rem(z_index - j + Z_PARTS, Z_PARTS) * pieces, pieces, axis
        )
        for j in range(Z_PARTS)
    ]
    return jnp.concatenate(parts, axis=axis)


def swap_x(values):
    return lax.ppermute(values, "head", [(h, h ^ 2) for h in range(4)])


def swap_core(values):
    return lax.ppermute(values, "head", [(h, h ^ 1) for h in range(4)])


def swap_y(values):
    return lax.ppermute(values, "blk", [(b, b ^ 1) for b in range(2 * Z_PARTS)])


def shift_z(values, amount):
    total = 2 * Z_PARTS
    return lax.ppermute(values, "blk", [(b, (b + 2 * amount) % total) for b in range(total)])


def swap_low_z(values):
    return lax.ppermute(values, "blk", [(b, b ^ 2) for b in range(2 * Z_PARTS)])


def gather_rows(own):
    half = own.shape[0] // 2
    from_x = swap_x(own)
    from_y = swap_y(own)
    corner_a = swap_y(from_x[:half])
    corner_b = swap_x(from_y[half:])
    mine = jnp.concatenate([own, from_y, from_x, corner_a, corner_b], axis=0)
    return jnp.concatenate([mine, swap_core(mine)], axis=0)


def scatter_rows(partial):
    rows = partial.shape[0] // 8
    half = rows // 2
    mine = partial[: 4 * rows]
    theirs = swap_core(partial[4 * rows :].astype(jnp.bfloat16))
    total = mine + theirs.astype(jnp.float32)
    own, for_y, for_x, corner = [total[i * rows : (i + 1) * rows] for i in range(4)]
    corner_b = corner.astype(jnp.bfloat16)
    got_x = swap_x(corner_b[:half]).astype(jnp.float32)
    got_y = swap_y(corner_b[half:]).astype(jnp.float32)
    for_y = jnp.concatenate([for_y[:half] + got_x, for_y[half:]], axis=0)
    for_x = jnp.concatenate([for_x[:half], for_x[half:] + got_y], axis=0)
    last_x = swap_x(for_x.astype(jnp.bfloat16)).astype(jnp.float32)
    last_y = swap_y(for_y.astype(jnp.bfloat16)).astype(jnp.float32)
    return own + last_x + last_y


def halve(values, bit, swap):
    mine = lax.dynamic_index_in_dim(values, bit, axis=0, keepdims=False)
    theirs = lax.dynamic_index_in_dim(values, 1 - bit, axis=0, keepdims=False)
    return mine + swap(theirs)


def scatter_sums(sums, x_index, core_index, z_index, y_index):
    count, width = sums.shape
    total = sums.reshape(count, 2, 2, 2, 2, 2, width // 32).transpose(1, 2, 3, 4, 5, 0, 6)
    total = halve(total, x_index, swap_x)
    total = halve(total, core_index, swap_core)
    total = halve(total, z_index // 2, lambda v: shift_z(v, 2))
    total = halve(total, z_index % 2, swap_low_z)
    return halve(total, y_index, swap_y)


def ring_gather(chunk, amount):
    held = [chunk]
    for unused in range(Z_PARTS - 1):
        held.append(shift_z(held[-1], amount))
    if amount == 1:
        return held
    return [held[(Z_PARTS - j) % Z_PARTS] for j in range(Z_PARTS)]


def ring_scatter(partials, amount):
    order = [(j + 1) % Z_PARTS for j in range(Z_PARTS)]
    if amount == -1:
        order = [(Z_PARTS - j) % Z_PARTS for j in order]
    total = partials[order[0]]
    for j in order[1:]:
        total = shift_z(total.astype(jnp.bfloat16), amount).astype(jnp.float32) + partials[j]
    return total


def to_even_odd(mine, theirs, y_index):
    got = swap_y(theirs)
    return jnp.where(y_index == 0, mine, got), jnp.where(y_index == 0, got, mine)


def from_even_odd(even, odd, y_index):
    mine = jnp.where(y_index == 0, even, odd)
    theirs = jnp.where(y_index == 0, odd, even).astype(jnp.bfloat16)
    got = swap_y(theirs).astype(jnp.float32)
    return jnp.where(y_index == 0, mine, got), jnp.where(y_index == 0, got, mine)


def to_heads(pieces, z_index):
    received = []
    for t in range(Z_PARTS):
        piece = lax.dynamic_index_in_dim(
            pieces, lax.rem(z_index + t, Z_PARTS), axis=0, keepdims=False
        )
        received.append(piece if t == 0 else shift_z(piece, t))
    return jnp.stack(received, axis=0)


def from_heads(pieces, z_index):
    received = [pieces[0]] + [shift_z(pieces[t], -t) for t in range(1, Z_PARTS)]
    ordered = jnp.stack(received + received, axis=0)
    return lax.dynamic_slice_in_dim(ordered, Z_PARTS - z_index, Z_PARTS, axis=0)


def tile_mask(key_tile, query_tile, start_row):
    key_pos = key_tile * KEY_TILE + lax.broadcasted_iota(jnp.int32, (KEY_TILE, QUERY_TILE), 0)
    query_pos = query_tile * QUERY_TILE + lax.broadcasted_iota(
        jnp.int32, (KEY_TILE, QUERY_TILE), 1
    )
    return (key_pos <= query_pos) & (key_pos >= start_row)


def mm(left, right, left_dim=1, right_dim=0):
    return lax.dot_general(
        left, right, (((left_dim,), (right_dim,)), ((), ())), preferred_element_type=jnp.float32
    )


def pack_blocks(slot_ref, source_ref, target_ref, blocks):
    per_part = source_ref.shape[2] // BLOCK
    for block in range(blocks):
        slot = slot_ref[block]
        part = slot // per_part
        column = pl.multiple_of((slot % per_part) * BLOCK, BLOCK)
        target_ref[:, block * BLOCK : (block + 1) * BLOCK] = source_ref[
            part, :, pl.ds(column, BLOCK)
        ]


def attend_kernel(
    slot_ref, low_ref, qkv_ref, start_ref, out_ref, exact_ref, norm_ref, packed_ref, keys_ref
):
    total = packed_ref.shape[1]
    blocks = total // BLOCK
    pack_blocks(slot_ref, qkv_ref, packed_ref, blocks)
    for tile in range(total // KEY_TILE):
        spot = slice(tile * KEY_TILE, (tile + 1) * KEY_TILE)
        keys_ref[spot, :] = packed_ref[HD : 2 * HD, spot].T

    def query_step(query_tile, unused):
        column = pl.multiple_of(query_tile * QUERY_TILE, QUERY_TILE)
        queries = packed_ref[0:HD, pl.ds(column, QUERY_TILE)] * HD ** (-0.5)
        queries = queries.astype(jnp.bfloat16)
        start_row = start_ref[:, pl.ds(column, QUERY_TILE)]

        def key_step(key_tile, state):
            run_max, run_sum, run_out = state
            row = pl.multiple_of(key_tile * KEY_TILE, KEY_TILE)
            scores = mm(keys_ref[pl.ds(row, KEY_TILE), :], queries)
            scores = jnp.where(tile_mask(key_tile, query_tile, start_row), scores, MASKED)
            new_max = jnp.maximum(run_max, jnp.max(scores, axis=0, keepdims=True))
            probs = jnp.exp(scores - new_max)
            fade = jnp.exp(run_max - new_max)
            run_sum = run_sum * fade + jnp.sum(probs, axis=0, keepdims=True)
            run_out = run_out * fade + mm(
                packed_ref[2 * HD : 3 * HD, pl.ds(row, KEY_TILE)], probs.astype(jnp.bfloat16)
            )
            return new_max, run_sum, run_out

        first = (
            jnp.full((1, QUERY_TILE), -3e38, jnp.float32),
            jnp.zeros((1, QUERY_TILE), jnp.float32),
            jnp.zeros((HD, QUERY_TILE), jnp.float32),
        )
        run_max, run_sum, run_out = lax.fori_loop(
            low_ref[query_tile], ((query_tile + 1) * QUERY_TILE) // KEY_TILE, key_step, first
        )
        exact_ref[:, pl.ds(column, QUERY_TILE)] = run_out / run_sum
        norm_ref[:, pl.ds(column, QUERY_TILE)] = run_max + jnp.log(run_sum)
        return unused

    lax.fori_loop(0, total // QUERY_TILE, query_step, 0)
    per_part = out_ref.shape[2] // BLOCK
    for block in range(blocks):
        slot = slot_ref[block]
        column = pl.multiple_of((slot % per_part) * BLOCK, BLOCK)
        out_ref[slot // per_part, :, pl.ds(column, BLOCK)] = exact_ref[
            :, block * BLOCK : (block + 1) * BLOCK
        ].astype(jnp.bfloat16)


def rotate_back(values, cosine, sine_table):
    half_rot = ROT // 2
    lead_part = values[0:half_rot]
    tail_part = values[half_rot:ROT]
    return jnp.concatenate(
        [
            lead_part * cosine + tail_part * sine_table,
            tail_part * cosine - lead_part * sine_table,
            values[ROT:],
        ],
        axis=0,
    )


def attend_back_kernel(
    slot_ref,
    low_ref,
    grad_ref,
    packed_ref,
    exact_ref,
    norm_ref,
    start_ref,
    cosine_ref,
    sine_ref,
    out_ref,
    bias_ref,
    keys_ref,
    values_ref,
    grads_ref,
    sums_ref,
):
    total = packed_ref.shape[1]
    blocks = total // BLOCK
    scale = HD ** (-0.5)
    pack_blocks(slot_ref, grad_ref, grads_ref, blocks)
    for tile in range(total // KEY_TILE):
        spot = slice(tile * KEY_TILE, (tile + 1) * KEY_TILE)
        keys_ref[spot, :] = packed_ref[HD : 2 * HD, spot].T
        values_ref[spot, :] = packed_ref[2 * HD : 3 * HD, spot].T
    sums_ref[HD : 3 * HD, :] = jnp.zeros((2 * HD, total), jnp.float32)

    def query_step(query_tile, unused):
        column = pl.multiple_of(query_tile * QUERY_TILE, QUERY_TILE)
        spot = pl.ds(column, QUERY_TILE)
        queries = (packed_ref[0:HD, spot] * scale).astype(jnp.bfloat16)
        grads = grads_ref[:, spot]
        start_row = start_ref[:, spot]
        norm_row = norm_ref[:, spot]
        delta_row = jnp.sum(
            grads.astype(jnp.float32) * exact_ref[:, spot], axis=0, keepdims=True
        )

        def key_step(key_tile, grad_query):
            row = pl.multiple_of(key_tile * KEY_TILE, KEY_TILE)
            rows = pl.ds(row, KEY_TILE)
            scores = mm(keys_ref[rows, :], queries)
            scores = jnp.where(tile_mask(key_tile, query_tile, start_row), scores, MASKED)
            probs = jnp.exp(scores - norm_row)
            grad_probs = mm(values_ref[rows, :], grads)
            grad_scores = (probs * (grad_probs - delta_row)).astype(jnp.bfloat16)
            probs_b = probs.astype(jnp.bfloat16)
            sums_ref[2 * HD : 3 * HD, rows] += mm(grads, probs_b, 1, 1)
            sums_ref[HD : 2 * HD, rows] += mm(queries, grad_scores, 1, 1)
            return grad_query + mm(packed_ref[HD : 2 * HD, rows], grad_scores)

        grad_query = lax.fori_loop(
            low_ref[query_tile],
            ((query_tile + 1) * QUERY_TILE) // KEY_TILE,
            key_step,
            jnp.zeros((HD, QUERY_TILE), jnp.float32),
        )
        sums_ref[0:HD, spot] = grad_query * scale
        return unused

    lax.fori_loop(0, total // QUERY_TILE, query_step, 0)
    per_part = out_ref.shape[2] // BLOCK
    bias_sum = jnp.zeros((3 * HD, BLOCK), jnp.float32)
    for block in range(blocks):
        spot = slice(block * BLOCK, (block + 1) * BLOCK)
        cosine = cosine_ref[:, spot]
        sine_table = sine_ref[:, spot]
        slot = slot_ref[block]
        column = pl.multiple_of((slot % per_part) * BLOCK, BLOCK)
        rounded = jnp.concatenate(
            [
                rotate_back(sums_ref[0:HD, spot], cosine, sine_table),
                rotate_back(sums_ref[HD : 2 * HD, spot], cosine, sine_table),
                sums_ref[2 * HD : 3 * HD, spot],
            ],
            axis=0,
        ).astype(jnp.bfloat16)
        out_ref[slot // per_part, :, pl.ds(column, BLOCK)] = rounded
        bias_sum = bias_sum + rounded.astype(jnp.float32)
    bias_ref[...] = bias_sum


def attend_heads(slot_of, low_tile, qkv_parts, start_row):
    parts, features, part_rows = qkv_parts.shape
    total = parts * part_rows
    vmem = pl.BlockSpec(memory_space=pltpu.VMEM)
    return pl.pallas_call(
        attend_kernel,
        grid_spec=pltpu.PrefetchScalarGridSpec(
            num_scalar_prefetch=2,
            grid=(1,),
            in_specs=[vmem, vmem],
            out_specs=[vmem, vmem, vmem, vmem],
            scratch_shapes=[pltpu.VMEM((total, HD), jnp.bfloat16)],
        ),
        out_shape=[
            jax.ShapeDtypeStruct((parts, HD, part_rows), jnp.bfloat16),
            jax.ShapeDtypeStruct((HD, total), jnp.float32),
            jax.ShapeDtypeStruct((1, total), jnp.float32),
            jax.ShapeDtypeStruct((3 * HD, total), jnp.bfloat16),
        ],
        cost_estimate=pl.CostEstimate(
            flops=total * total * HD, transcendentals=total * total // 4, bytes_accessed=6 << 20
        ),
        compiler_params=pltpu.CompilerParams(vmem_limit_bytes=40 << 20),
        name="attend",
    )(slot_of, low_tile, qkv_parts, start_row)


def attend_heads_back(
    slot_of, low_tile, grad_parts, packed, exact, log_norm, start_row, cosine, sine_table
):
    parts, features, part_rows = grad_parts.shape
    total = parts * part_rows
    vmem = pl.BlockSpec(memory_space=pltpu.VMEM)
    return pl.pallas_call(
        attend_back_kernel,
        grid_spec=pltpu.PrefetchScalarGridSpec(
            num_scalar_prefetch=2,
            grid=(1,),
            in_specs=[vmem] * 7,
            out_specs=[vmem, vmem],
            scratch_shapes=[
                pltpu.VMEM((total, HD), jnp.bfloat16),
                pltpu.VMEM((total, HD), jnp.bfloat16),
                pltpu.VMEM((HD, total), jnp.bfloat16),
                pltpu.VMEM((3 * HD, total), jnp.float32),
            ],
        ),
        out_shape=[
            jax.ShapeDtypeStruct((parts, 3 * HD, part_rows), jnp.bfloat16),
            jax.ShapeDtypeStruct((3 * HD, BLOCK), jnp.float32),
        ],
        cost_estimate=pl.CostEstimate(
            flops=3 * total * total * HD,
            transcendentals=total * total // 4,
            bytes_accessed=8 << 20,
        ),
        compiler_params=pltpu.CompilerParams(vmem_limit_bytes=50 << 20),
        name="attend_back",
    )(slot_of, low_tile, grad_parts, packed, exact, log_norm, start_row, cosine, sine_table)


def start_of(position, seq_lengths):
    seq_ends = jnp.cumsum(seq_lengths)
    ends_before = seq_ends[:, None] <= position[None, :]
    return jnp.sum(jnp.where(ends_before, seq_lengths[:, None], 0), axis=0)


def rotary_tables(offset_in_seq):
    half_rot = ROT // 2
    freq_table = jnp.power(10000.0, -2.0 * jnp.arange(half_rot, dtype=jnp.float32) / ROT)
    angles = freq_table[:, None] * offset_in_seq.astype(jnp.float32)[None, :]
    return jnp.cos(angles), jnp.sin(angles)


def on_device_heads(
    tokens,
    norm1_gain,
    norm1_bias,
    w_qkv,
    qkv_bias,
    w_out,
    norm2_gain,
    norm2_bias,
    w_gate,
    w_up,
    w_down,
    cotangent,
    seq_lengths,
    block_order,
):
    head_index = lax.axis_index("head")
    blk_index = lax.axis_index("blk")
    x_index, core_index = head_index // 2, head_index % 2
    z_index, y_index = blk_index // 2, blk_index % 2
    tok_rows, model_width = tokens.shape
    plane_rows = 8 * tok_rows
    total_rows = Z_PARTS * plane_rows
    row_block = model_width // (2 * Z_PARTS)
    chunk = 2 * row_block
    ff_half = w_gate.shape[1] // 2
    heads_width = Z_PARTS * HD

    qkv_split = w_qkv.reshape(row_block, 3, Z_PARTS, 2, HD)
    qkv_low = qkv_split[:, :, :, 0].reshape(row_block, 3 * heads_width)
    qkv_high = qkv_split[:, :, :, 1].reshape(row_block, 3 * heads_width)
    first = y_index == 0
    qkv_even, qkv_odd = to_even_odd(
        jnp.where(first, qkv_low, qkv_high), jnp.where(first, qkv_high, qkv_low), y_index
    )
    out_split = w_out.reshape(Z_PARTS, 2, HD, row_block)
    out_low = out_split[:, 0].reshape(heads_width, row_block)
    out_high = out_split[:, 1].reshape(heads_width, row_block)
    out_even, out_odd = to_even_odd(
        jnp.where(first, out_low, out_high), jnp.where(first, out_high, out_low), y_index
    )

    def column_halves(weight):
        low, high = weight[:, :ff_half], weight[:, ff_half:]
        return to_even_odd(jnp.where(first, low, high), jnp.where(first, high, low), y_index)

    gate_own = jnp.concatenate(column_halves(w_gate), axis=0)
    up_own = jnp.concatenate(column_halves(w_up), axis=0)
    down_low, down_high = w_down[:ff_half], w_down[ff_half:]
    down_even, down_odd = to_even_odd(
        jnp.where(first, down_low, down_high), jnp.where(first, down_high, down_low), y_index
    )

    def both_ways(even, odd, axis):
        forward = ring_gather(even, 1)
        backward = ring_gather(odd, -1)
        pieces = [p for pair in zip(forward, backward) for p in pair]
        return jnp.concatenate(pieces, axis=axis)

    x_own = split_order(tokens, z_index, 1).astype(jnp.float32)
    gain_one = split_order(norm1_gain, z_index, 0)
    shift_one = split_order(norm1_bias, z_index, 0)
    gain_two = split_order(norm2_gain, z_index, 0)
    shift_two = split_order(norm2_bias, z_index, 0)
    norm1_out, unit_one, inv_one = normalize(x_own, gain_one, shift_one)
    norm1_all = gather_rows(norm1_out.astype(jnp.bfloat16))
    qkv_full = both_ways(qkv_even, qkv_odd, 0)
    out_full = both_ways(out_even, out_odd, 1)
    gate_full = jnp.concatenate(ring_gather(gate_own, 1), axis=0)
    up_full = jnp.concatenate(ring_gather(up_own, -1), axis=0)
    down_full = both_ways(down_even, down_odd, 1)

    slots = jnp.arange(Z_PARTS * 8, dtype=jnp.int32)
    step_z, flip = slots // 8, slots % 8
    owner = (
        ((x_index ^ ((flip // 2) % 2)) * 2 + (core_index ^ (flip // 4))) * (2 * Z_PARTS)
        + ((z_index - step_z + Z_PARTS) % Z_PARTS) * 2
        + (y_index ^ (flip % 2))
    )
    packed_block = jnp.sum(
        jnp.where(owner[:, None] == slots[None, :], block_order[None, :], 0), axis=1
    )
    slot_of = jnp.sum(
        jnp.where(packed_block[None, :] == slots[:, None], slots[None, :], 0), axis=1
    )
    plane_pos = (
        packed_block[:8, None] * BLOCK + jnp.arange(BLOCK, dtype=jnp.int32)[None, :]
    ).reshape(-1)
    plane_cos, plane_sin = rotary_tables(plane_pos - start_of(plane_pos, seq_lengths))
    all_pos = jnp.arange(total_rows, dtype=jnp.int32)
    all_start = start_of(all_pos, seq_lengths)
    all_cos, all_sin = rotary_tables(all_pos - all_start)
    low_tile = (
        start_of(
            jnp.arange(total_rows // QUERY_TILE, dtype=jnp.int32) * QUERY_TILE, seq_lengths
        )
        // KEY_TILE
    )
    start_row = all_start[None, :]

    bias_split = qkv_bias.reshape(3, Z_PARTS, 2, HD)
    bias_own = jnp.where(first, bias_split[:, :, 0], bias_split[:, :, 1]).reshape(-1)
    projected = (mm(qkv_full, norm1_all, 0, 1) + bias_own[:, None]).reshape(
        3, Z_PARTS, HD, plane_rows
    )
    half_rot = ROT // 2
    lead_part, tail_part = projected[:2, :, :half_rot], projected[:2, :, half_rot:ROT]
    rotated = jnp.concatenate(
        [
            lead_part * plane_cos - tail_part * plane_sin,
            tail_part * plane_cos + lead_part * plane_sin,
            projected[:2, :, ROT:],
        ],
        axis=2,
    )
    qkv_heads = jnp.concatenate([rotated, projected[2:]], axis=0).astype(jnp.bfloat16)
    qkv_heads = qkv_heads.transpose(1, 0, 2, 3).reshape(Z_PARTS, 3 * HD, plane_rows)
    qkv_parts = to_heads(qkv_heads, z_index)
    attn_parts, attn_exact, log_norm, packed = attend_heads(
        slot_of, low_tile, qkv_parts, start_row
    )
    attn_t = from_heads(attn_parts, z_index).reshape(heads_width, plane_rows)
    attn_own = scatter_rows(mm(attn_t, out_full, 0, 0))

    hidden = x_own + attn_own
    norm2_out, unit_two, inv_two = normalize(hidden, gain_two, shift_two)
    norm2_all = gather_rows(norm2_out.astype(jnp.bfloat16))
    cotangent_own = split_order(cotangent, z_index, 1)
    grad_all = gather_rows(cotangent_own)
    gate_val = mm(norm2_all, gate_full)
    up_val = mm(norm2_all, up_full)
    sigmoid_gate = jax.nn.sigmoid(gate_val)
    swish_val = gate_val * sigmoid_gate
    activ_b = (swish_val * up_val).astype(jnp.bfloat16)
    grad_activ = mm(grad_all, down_full, 1, 1)
    grad_up_b = (grad_activ * swish_val).astype(jnp.bfloat16)
    grad_gate_b = (
        grad_activ * up_val * sigmoid_gate * (1.0 + gate_val * (1.0 - sigmoid_gate))
    ).astype(jnp.bfloat16)
    grad_norm2 = scatter_rows(mm(grad_gate_b, gate_full, 1, 1) + mm(grad_up_b, up_full, 1, 1))
    mlp_own = scatter_rows(mm(activ_b, down_full))
    output = split_order((hidden + mlp_own).astype(jnp.bfloat16), z_index, 1)

    def pieces_of(values, width, offset=0, size=None):
        size = width if size is None else size
        return [
            values[:, j * width + offset : j * width + offset + size] for j in range(Z_PARTS)
        ]

    down_sum_even = ring_scatter(
        [mm(activ_b, p, 0, 0) for p in pieces_of(grad_all, chunk, 0, row_block)], 1
    )
    down_sum_odd = ring_scatter(
        [mm(activ_b, p, 0, 0) for p in pieces_of(grad_all, chunk, row_block, row_block)], -1
    )
    down_parts = from_even_odd(down_sum_even, down_sum_odd, y_index)
    down_grad = jnp.concatenate(down_parts, axis=0)
    gate_sum = ring_scatter([mm(p, grad_gate_b, 0, 0) for p in pieces_of(norm2_all, chunk)], 1)
    up_sum = ring_scatter([mm(p, grad_up_b, 0, 0) for p in pieces_of(norm2_all, chunk)], -1)
    gate_grad = jnp.concatenate(
        from_even_odd(gate_sum[:row_block], gate_sum[row_block:], y_index), axis=1
    )
    up_grad = jnp.concatenate(
        from_even_odd(up_sum[:row_block], up_sum[row_block:], y_index), axis=1
    )

    grad_out = cotangent_own.astype(jnp.float32)
    grad_hidden = grad_out + normalize_back(grad_norm2, unit_two, inv_two, gain_two)
    branch_all = gather_rows(grad_hidden.astype(jnp.bfloat16))
    grad_attn = (
        mm(out_full, branch_all, 1, 1)
        .astype(jnp.bfloat16)
        .reshape(Z_PARTS, HD, plane_rows)
    )
    grad_parts = to_heads(grad_attn, z_index)
    proj_parts, bias_sums = attend_heads_back(
        slot_of, low_tile, grad_parts, packed, attn_exact, log_norm, start_row, all_cos, all_sin
    )
    bias_grad = jnp.sum(bias_sums, axis=1).reshape(3, HD)
    grad_proj = from_heads(proj_parts, z_index).reshape(Z_PARTS, 3, HD, plane_rows)
    grad_proj = grad_proj.transpose(1, 0, 2, 3).reshape(3 * heads_width, plane_rows)
    grad_norm1 = scatter_rows(mm(grad_proj, qkv_full, 0, 1))

    out_sum_even = ring_scatter(
        [mm(attn_t, p) for p in pieces_of(branch_all, chunk, 0, row_block)], 1
    )
    out_sum_odd = ring_scatter(
        [mm(attn_t, p) for p in pieces_of(branch_all, chunk, row_block, row_block)], -1
    )
    out_parts = from_even_odd(out_sum_even, out_sum_odd, y_index)
    out_grad = jnp.stack(
        [p.reshape(Z_PARTS, HD, row_block) for p in out_parts], axis=1
    ).reshape(w_out.shape)
    qkv_sum_even = ring_scatter(
        [mm(p, grad_proj, 0, 1) for p in pieces_of(norm1_all, chunk, 0, row_block)], 1
    )
    qkv_sum_odd = ring_scatter(
        [mm(p, grad_proj, 0, 1) for p in pieces_of(norm1_all, chunk, row_block, row_block)], -1
    )
    qkv_grad_parts = from_even_odd(qkv_sum_even, qkv_sum_odd, y_index)
    qkv_grad = jnp.stack(
        [p.reshape(row_block, 3, Z_PARTS, HD) for p in qkv_grad_parts], axis=3
    ).reshape(w_qkv.shape)

    input_grad = grad_hidden + normalize_back(grad_norm1, unit_one, inv_one, gain_one)
    sums = jnp.stack(
        [
            jnp.sum(grad_norm1 * unit_one, axis=0),
            jnp.sum(grad_norm1, axis=0),
            jnp.sum(grad_norm2 * unit_two, axis=0),
            jnp.sum(grad_norm2, axis=0),
        ],
        axis=0,
    )
    norm_sums = scatter_sums(
        split_order(sums, z_index, 1), x_index, core_index, z_index, y_index
    )
    return (
        output,
        split_order(input_grad, z_index, 1),
        norm_sums[0],
        norm_sums[1],
        qkv_grad,
        bias_grad,
        out_grad,
        norm_sums[2],
        norm_sums[3],
        gate_grad,
        up_grad,
        down_grad,
    )


def solution(mesh):
    placed = (
        P(("head", "blk"), None),
        P(),
        P(),
        P("blk", None, "head"),
        P(None, "head"),
        P("head", "blk"),
        P(),
        P(),
        P("blk", "head"),
        P("blk", "head"),
        P("head", "blk"),
        P(("head", "blk"), None),
        P(),
        P(),
    )
    heads_plan = mesh.shape["head"] == 4 and mesh.shape["blk"] == 2 * Z_PARTS
    return jax.shard_map(
        on_device_heads if heads_plan else on_device,
        mesh=mesh,
        in_specs=placed,
        out_specs=(
            P(("head", "blk"), None),
            P(("head", "blk"), None),
            P(("head", "blk")),
            P(("head", "blk")),
            P("blk", None, "head"),
            P(None, ("head", "blk")),
            P("head", "blk"),
            P(("head", "blk")),
            P(("head", "blk")),
            P("blk", "head"),
            P("blk", "head"),
            P("head", "blk"),
        ),
        check_vma=False,
    )
```

```python
import jax
import jax.numpy as jnp
from jax import lax
from jax.experimental import pallas as pl
from jax.experimental.pallas import tpu as pltpu
from jax.sharding import PartitionSpec as P


HD = 64
ROT = 16
BLOCK = 128
Z_PARTS = 4
QUERY_TILE = 512
KEY_TILE = 256


EPSILON = 1e-05
MASKED = -1000000000.0


def contract_rows(left, right):
    return lax.dot_general(
        left, right, (((0,), (0,)), ((), ())), preferred_element_type=jnp.float32
    )


def times_transpose(left, right):
    return lax.dot_general(
        left, right, (((1,), (1,)), ((), ())), preferred_element_type=jnp.float32
    )


def packed_positions(row_ids, block_order):
    block_ids = jnp.arange(block_order.shape[0], dtype=jnp.int32)
    matches = (row_ids // BLOCK)[:, None] == block_ids[None, :]
    block_start = jnp.sum(jnp.where(matches, block_order[None, :], 0), axis=1)
    return block_start * BLOCK + row_ids % BLOCK


def sequence_start(position, seq_lengths):
    seq_ends = jnp.cumsum(seq_lengths)
    ends_before = seq_ends[None, :] <= position[:, None]
    return jnp.sum(jnp.where(ends_before, seq_lengths[None, :], 0), axis=1)


def rotate(values, cosine, sine_table):
    half_rot = ROT // 2
    lead_part = values[..., :half_rot]
    tail_part = values[..., half_rot:ROT]
    cos_rows = cosine[:, None, :]
    sin_rows = sine_table[:, None, :]
    return jnp.concatenate(
        [
            lead_part * cos_rows - tail_part * sin_rows,
            tail_part * cos_rows + lead_part * sin_rows,
            values[..., ROT:],
        ],
        axis=-1,
    )


def normalize(values, norm_gain, norm_shift):
    centre = values - jnp.mean(values, axis=-1, keepdims=True)
    inv_scale = lax.rsqrt(jnp.mean(centre * centre, axis=-1, keepdims=True) + EPSILON)
    unit_rows = centre * inv_scale
    return (unit_rows * norm_gain + norm_shift, unit_rows, inv_scale)


def normalize_back(grad_norm, unit_rows, inv_scale, norm_gain):
    grad_unit = grad_norm * norm_gain
    mean_grad = jnp.mean(grad_unit, axis=-1, keepdims=True)
    mean_proj = jnp.mean(grad_unit * unit_rows, axis=-1, keepdims=True)
    return inv_scale * (grad_unit - mean_grad - unit_rows * mean_proj)


def gather_keys(keys_flat, values_flat):
    return (
        lax.all_gather(keys_flat, "blk", axis=0, tiled=True),
        lax.all_gather(values_flat, "blk", axis=0, tiled=True),
    )


def tile_count_of(total_rows):
    tile_rows = min(1024, total_rows)
    return (total_rows // tile_rows, tile_rows)


def key_tiles(keys_all, values_all, key_pos, heads_local):
    tile_count, tile_rows = tile_count_of(keys_all.shape[0])
    return (
        keys_all.reshape(tile_count, tile_rows, heads_local, HD),
        values_all.reshape(tile_count, tile_rows, heads_local, HD),
        key_pos.reshape(tile_count, tile_rows),
    )


def masked_scores(queries, key_tile, pos_tile, query_pos, query_start):
    raw_scores = jnp.einsum(
        "qhd,khd->hqk", queries, key_tile, preferred_element_type=jnp.float32
    ) * HD ** (-0.5)
    allowed = (pos_tile[None, :] <= query_pos[:, None]) & (
        pos_tile[None, :] >= query_start[:, None]
    )
    return jnp.where(allowed[None], raw_scores, MASKED)


def attend(queries, tiles, query_pos, query_start):
    group_rows = queries.shape[0]
    heads_local = queries.shape[1]

    def first_pass(run_state, tile):
        run_max, run_sum = run_state
        scores = masked_scores(queries, tile[0], tile[2], query_pos, query_start)
        new_max = jnp.maximum(run_max, jnp.max(scores, axis=-1))
        new_sum = run_sum * jnp.exp(run_max - new_max) + jnp.sum(
            jnp.exp(scores - new_max[..., None]), axis=-1
        )
        return ((new_max, new_sum), None)

    start_state = (
        jnp.full((heads_local, group_rows), -3e38, jnp.float32),
        jnp.zeros((heads_local, group_rows), jnp.float32),
    )
    (run_max, run_sum), unused = lax.scan(first_pass, start_state, tiles)
    log_norm = run_max + jnp.log(run_sum)

    def second_pass(totals, tile):
        total_out, total_rest = totals
        scores = masked_scores(queries, tile[0], tile[2], query_pos, query_start)
        probs_f32 = jnp.exp(scores - log_norm[..., None])
        probs_b = probs_f32.astype(jnp.bfloat16)
        rest_b = (probs_f32 - probs_b.astype(jnp.float32)).astype(jnp.bfloat16)
        total_out = total_out + jnp.einsum(
            "hqk,khd->qhd", probs_b, tile[1], preferred_element_type=jnp.float32
        )
        total_rest = total_rest + jnp.einsum(
            "hqk,khd->qhd", rest_b, tile[1], preferred_element_type=jnp.float32
        )
        return ((total_out, total_rest), None)

    empty = jnp.zeros((group_rows, heads_local, HD), jnp.float32)
    (attended, leftover), unused = lax.scan(second_pass, (empty, empty), tiles)
    return (attended, attended + leftover, log_norm)


def attend_back(queries, tiles, query_pos, query_start, log_norm, grad_attn, delta_rows):
    scale = HD ** (-0.5)

    def step_back(grad_query, tile):
        key_tile, value_tile, pos_tile = tile
        scores = masked_scores(queries, key_tile, pos_tile, query_pos, query_start)
        probs_f32 = jnp.exp(scores - log_norm[..., None])
        grad_probs = jnp.einsum(
            "qhd,khd->hqk", grad_attn, value_tile, preferred_element_type=jnp.float32
        )
        grad_scores = (probs_f32 * (grad_probs - delta_rows[..., None])).astype(jnp.bfloat16)
        probs_b = probs_f32.astype(jnp.bfloat16)
        grad_query = grad_query + scale * jnp.einsum(
            "hqk,khd->qhd", grad_scores, key_tile, preferred_element_type=jnp.float32
        )
        grad_key = scale * jnp.einsum(
            "hqk,qhd->khd", grad_scores, queries, preferred_element_type=jnp.float32
        )
        grad_value = jnp.einsum(
            "hqk,qhd->khd", probs_b, grad_attn, preferred_element_type=jnp.float32
        )
        return (grad_query, (grad_key, grad_value))

    grad_query, (grad_keys, grad_values) = lax.scan(
        step_back, jnp.zeros(queries.shape, jnp.float32), tiles
    )
    return (grad_query, grad_keys, grad_values)


def on_device(
    tokens,
    norm1_gain,
    norm1_bias,
    w_qkv,
    qkv_bias,
    w_out,
    norm2_gain,
    norm2_bias,
    w_gate,
    w_up,
    w_down,
    cotangent,
    seq_lengths,
    block_order,
):
    team_count = lax.axis_size("head")
    span_count = lax.axis_size("blk")
    span_index = lax.axis_index("blk")
    tok_rows = tokens.shape[0]
    model_width = tokens.shape[1]
    group_rows = tok_rows * team_count
    local_width = w_out.shape[0]
    heads_local = local_width // HD
    offsets = jnp.arange(tok_rows, dtype=jnp.int32)
    member = jnp.arange(team_count, dtype=jnp.int32)
    owner_index = jnp.arange(span_count, dtype=jnp.int32)
    query_ids = ((member[:, None] * span_count + span_index) * tok_rows + offsets[None, :]).reshape(
        -1
    )
    key_ids = (
        (member[None, :, None] * span_count + owner_index[:, None, None]) * tok_rows
        + offsets[None, None, :]
    ).reshape(-1)
    query_pos = packed_positions(query_ids, block_order)
    query_start = sequence_start(query_pos, seq_lengths)
    key_pos = packed_positions(key_ids, block_order)
    half_rot = ROT // 2
    freq_table = jnp.power(10000.0, -2.0 * jnp.arange(half_rot, dtype=jnp.float32) / ROT)
    angles = (query_pos - query_start).astype(jnp.float32)[:, None] * freq_table[None, :]
    cosine = jnp.cos(angles)
    sine_table = jnp.sin(angles)
    x_own = tokens.astype(jnp.float32)
    norm1_out, unit_one, inv_one = normalize(x_own, norm1_gain, norm1_bias)
    norm1_group = lax.all_gather(norm1_out.astype(jnp.bfloat16), "head", axis=0, tiled=True)
    qkv_full, out_full = (
        lax.all_gather(w_qkv, "blk", axis=0, tiled=True),
        lax.all_gather(w_out, "blk", axis=1, tiled=True),
    )
    qkv_matrix = qkv_full.reshape(model_width, 3 * local_width)
    projected = jnp.dot(
        norm1_group, qkv_matrix, preferred_element_type=jnp.float32
    ) + qkv_bias.reshape(1, -1)
    projected = projected.reshape(group_rows, 3, heads_local, HD)
    queries = rotate(projected[:, 0], cosine, sine_table).astype(jnp.bfloat16)
    keys_flat = (
        rotate(projected[:, 1], cosine, sine_table)
        .astype(jnp.bfloat16)
        .reshape(group_rows, local_width)
    )
    values_flat = projected[:, 2].astype(jnp.bfloat16).reshape(group_rows, local_width)
    keys_all, values_all = gather_keys(keys_flat, values_flat)
    attn_out, attn_exact, log_norm = attend(
        queries, key_tiles(keys_all, values_all, key_pos, heads_local), query_pos, query_start
    )
    attn_b = attn_out.reshape(group_rows, local_width).astype(jnp.bfloat16)
    attn_own = lax.psum_scatter(
        jnp.dot(attn_b, out_full, preferred_element_type=jnp.float32),
        "head",
        scatter_dimension=0,
        tiled=True,
    )
    hidden = x_own + attn_own
    norm2_out, unit_two, inv_two = normalize(hidden, norm2_gain, norm2_bias)
    norm2_group = lax.all_gather(norm2_out.astype(jnp.bfloat16), "head", axis=0, tiled=True)
    gate_full, up_full, down_full = (
        lax.all_gather(w_gate, "blk", axis=0, tiled=True),
        lax.all_gather(w_up, "blk", axis=0, tiled=True),
        lax.all_gather(w_down, "blk", axis=1, tiled=True),
    )
    gate_val = jnp.dot(norm2_group, gate_full, preferred_element_type=jnp.float32)
    up_val = jnp.dot(norm2_group, up_full, preferred_element_type=jnp.float32)
    sigmoid_gate = jax.nn.sigmoid(gate_val)
    swish_val = gate_val * sigmoid_gate
    activ_b = (swish_val * up_val).astype(jnp.bfloat16)
    mlp_own = lax.psum_scatter(
        jnp.dot(activ_b, down_full, preferred_element_type=jnp.float32).astype(jnp.bfloat16),
        "head",
        scatter_dimension=0,
        tiled=True,
    ).astype(jnp.float32)
    output = (hidden + mlp_own).astype(jnp.bfloat16)
    grad_out = cotangent.astype(jnp.float32)
    grad_group = lax.all_gather(cotangent, "head", axis=0, tiled=True)
    grad_activ = times_transpose(grad_group, down_full)
    grad_w_down = contract_rows(activ_b, grad_group)
    grad_up_b = (grad_activ * swish_val).astype(jnp.bfloat16)
    grad_gate_b = (
        grad_activ * up_val * sigmoid_gate * (1.0 + gate_val * (1.0 - sigmoid_gate))
    ).astype(jnp.bfloat16)
    grad_w_gate = contract_rows(norm2_group, grad_gate_b)
    grad_w_up = contract_rows(norm2_group, grad_up_b)
    grad_norm2 = lax.psum_scatter(
        times_transpose(grad_gate_b, gate_full) + times_transpose(grad_up_b, up_full),
        "head",
        scatter_dimension=0,
        tiled=True,
    )
    grad_hidden = grad_out + normalize_back(grad_norm2, unit_two, inv_two, norm2_gain)
    gain_two_grad = jnp.sum(grad_norm2 * unit_two, axis=0)
    shift_two_grad = jnp.sum(grad_norm2, axis=0)
    branch_group = lax.all_gather(grad_hidden.astype(jnp.bfloat16), "head", axis=0, tiled=True)
    grad_w_out = contract_rows(attn_b, branch_group)
    grad_attn = (
        times_transpose(branch_group, out_full)
        .astype(jnp.bfloat16)
        .reshape(group_rows, heads_local, HD)
    )
    delta_rows = jnp.sum(grad_attn.astype(jnp.float32) * attn_exact, axis=-1).T
    keys_back_all, values_back_all = gather_keys(keys_flat, values_flat)
    tiles_back = key_tiles(keys_back_all, values_back_all, key_pos, heads_local)
    grad_query, grad_keys, grad_values = attend_back(
        queries, tiles_back, query_pos, query_start, log_norm, grad_attn, delta_rows
    )
    key_terms = grad_keys.reshape(-1, local_width)
    value_terms = grad_values.reshape(-1, local_width)
    grad_key_own, grad_value_own = (
        lax.psum_scatter(
            key_terms.astype(jnp.bfloat16), "blk", scatter_dimension=0, tiled=True
        ).astype(jnp.float32),
        lax.psum_scatter(
            value_terms.astype(jnp.bfloat16), "blk", scatter_dimension=0, tiled=True
        ).astype(jnp.float32),
    )
    grad_query_pre = rotate(grad_query, cosine, -sine_table).reshape(group_rows, local_width)
    grad_key_pre = rotate(
        grad_key_own.reshape(group_rows, heads_local, HD), cosine, -sine_table
    ).reshape(group_rows, local_width)
    grad_proj_b = jnp.stack([grad_query_pre, grad_key_pre, grad_value_own], axis=1).astype(
        jnp.bfloat16
    )
    bias_grad = jnp.sum(grad_proj_b.astype(jnp.float32), axis=0)
    grad_proj_flat = grad_proj_b.reshape(group_rows, 3 * local_width)
    grad_w_qkv = contract_rows(norm1_group, grad_proj_flat).reshape(model_width, 3, local_width)
    grad_norm1 = lax.psum_scatter(
        times_transpose(grad_proj_flat, qkv_matrix).astype(jnp.bfloat16),
        "head",
        scatter_dimension=0,
        tiled=True,
    ).astype(jnp.float32)
    input_grad = grad_hidden + normalize_back(grad_norm1, unit_one, inv_one, norm1_gain)
    gain_one_grad = jnp.sum(grad_norm1 * unit_one, axis=0)
    shift_one_grad = jnp.sum(grad_norm1, axis=0)
    norm_sums = (
        lax.psum_scatter(gain_one_grad, ("head", "blk"), scatter_dimension=0, tiled=True),
        lax.psum_scatter(shift_one_grad, ("head", "blk"), scatter_dimension=0, tiled=True),
        lax.psum_scatter(gain_two_grad, ("head", "blk"), scatter_dimension=0, tiled=True),
        lax.psum_scatter(shift_two_grad, ("head", "blk"), scatter_dimension=0, tiled=True),
    )
    grad_shards = (
        lax.psum_scatter(
            grad_w_qkv.astype(jnp.bfloat16), "blk", scatter_dimension=0, tiled=True
        ).astype(jnp.float32),
        lax.psum_scatter(
            bias_grad.astype(jnp.bfloat16), "blk", scatter_dimension=1, tiled=True
        ).astype(jnp.float32),
        lax.psum_scatter(
            grad_w_out.astype(jnp.bfloat16), "blk", scatter_dimension=1, tiled=True
        ).astype(jnp.float32),
        lax.psum_scatter(
            grad_w_gate.astype(jnp.bfloat16), "blk", scatter_dimension=0, tiled=True
        ).astype(jnp.float32),
        lax.psum_scatter(
            grad_w_up.astype(jnp.bfloat16), "blk", scatter_dimension=0, tiled=True
        ).astype(jnp.float32),
        lax.psum_scatter(
            grad_w_down.astype(jnp.bfloat16), "blk", scatter_dimension=1, tiled=True
        ).astype(jnp.float32),
    )
    return (
        output,
        input_grad,
        norm_sums[0],
        norm_sums[1],
        grad_shards[0],
        grad_shards[1],
        grad_shards[2],
        norm_sums[2],
        norm_sums[3],
        grad_shards[3],
        grad_shards[4],
        grad_shards[5],
    )


def split_order(values, z_index, axis):
    pieces = values.shape[axis] // Z_PARTS
    parts = [
        lax.dynamic_slice_in_dim(
            values, lax.rem(z_index - j + Z_PARTS, Z_PARTS) * pieces, pieces, axis
        )
        for j in range(Z_PARTS)
    ]
    return jnp.concatenate(parts, axis=axis)


def swap_x(values):
    return lax.ppermute(values, "head", [(h, h ^ 2) for h in range(4)])


def swap_core(values):
    return lax.ppermute(values, "head", [(h, h ^ 1) for h in range(4)])


def swap_y(values):
    return lax.ppermute(values, "blk", [(b, b ^ 1) for b in range(2 * Z_PARTS)])


def shift_z(values, amount):
    total = 2 * Z_PARTS
    return lax.ppermute(values, "blk", [(b, (b + 2 * amount) % total) for b in range(total)])


def swap_low_z(values):
    return lax.ppermute(values, "blk", [(b, b ^ 2) for b in range(2 * Z_PARTS)])


def gather_rows(own):
    half = own.shape[0] // 2
    from_x = swap_x(own)
    from_y = swap_y(own)
    corner_a = swap_y(from_x[:half])
    corner_b = swap_x(from_y[half:])
    mine = jnp.concatenate([own, from_y, from_x, corner_a, corner_b], axis=0)
    other = swap_core(mine)
    return jnp.concatenate([mine, other], axis=0)


def scatter_rows(partial):
    rows = partial.shape[0] // 8
    half = rows // 2
    mine = partial[: 4 * rows]
    theirs = swap_core(partial[4 * rows :].astype(jnp.bfloat16))
    total = mine + theirs.astype(jnp.float32)
    own, for_y, for_x, corner = [total[i * rows : (i + 1) * rows] for i in range(4)]
    corner_b = corner.astype(jnp.bfloat16)
    got_x = swap_x(corner_b[:half]).astype(jnp.float32)
    got_y = swap_y(corner_b[half:]).astype(jnp.float32)
    for_y = jnp.concatenate([for_y[:half] + got_x, for_y[half:]], axis=0)
    for_x = jnp.concatenate([for_x[:half], for_x[half:] + got_y], axis=0)
    last_x = swap_x(for_x.astype(jnp.bfloat16)).astype(jnp.float32)
    last_y = swap_y(for_y.astype(jnp.bfloat16)).astype(jnp.float32)
    return own + last_x + last_y


def halve(values, bit, swap):
    mine = lax.dynamic_index_in_dim(values, bit, axis=0, keepdims=False)
    theirs = lax.dynamic_index_in_dim(values, 1 - bit, axis=0, keepdims=False)
    return mine + swap(theirs)


def scatter_sums(sums, x_index, core_index, z_index, y_index):
    count, width = sums.shape
    total = sums.reshape(count, 2, 2, 2, 2, 2, width // 32).transpose(1, 2, 3, 4, 5, 0, 6)
    total = halve(total, x_index, swap_x)
    total = halve(total, core_index, swap_core)
    total = halve(total, z_index // 2, lambda v: shift_z(v, 2))
    total = halve(total, z_index % 2, swap_low_z)
    return halve(total, y_index, swap_y)


def ring_gather(chunk, amount):
    held = [chunk]
    for _ in range(1, Z_PARTS):
        held.append(shift_z(held[-1], amount))
    if amount == 1:
        return held
    return [held[(Z_PARTS - j) % Z_PARTS] for j in range(Z_PARTS)]


def ring_scatter(partials, amount):
    order = [(j + 1) % Z_PARTS for j in range(Z_PARTS)]
    if amount == -1:
        order = [(Z_PARTS - j) % Z_PARTS for j in order]
    total = partials[order[0]]
    for hop in range(1, Z_PARTS):
        moved = shift_z(total.astype(jnp.bfloat16), amount)
        total = moved.astype(jnp.float32) + partials[order[hop]]
    return total


def to_even_odd(mine, theirs, y_index):
    got = swap_y(theirs)
    return jnp.where(y_index == 0, mine, got), jnp.where(y_index == 0, got, mine)


def from_even_odd(even, odd, y_index):
    mine = jnp.where(y_index == 0, even, odd)
    theirs = jnp.where(y_index == 0, odd, even).astype(jnp.bfloat16)
    got = swap_y(theirs).astype(jnp.float32)
    return jnp.where(y_index == 0, mine, got), jnp.where(y_index == 0, got, mine)


def to_heads(pieces, z_index):
    received = []
    for t in range(Z_PARTS):
        piece = lax.dynamic_index_in_dim(
            pieces, lax.rem(z_index + t, Z_PARTS), axis=0, keepdims=False
        )
        received.append(piece if t == 0 else shift_z(piece, t))
    return jnp.stack(received, axis=0)


def from_heads(pieces, z_index):
    received = [pieces[0]] + [shift_z(pieces[t], -t) for t in range(1, Z_PARTS)]
    ordered = jnp.stack(received + received, axis=0)
    return lax.dynamic_slice_in_dim(ordered, Z_PARTS - z_index, Z_PARTS, axis=0)


def tile_mask(key_tile, query_tile, start_row):
    key_pos = key_tile * KEY_TILE + lax.broadcasted_iota(jnp.int32, (KEY_TILE, QUERY_TILE), 0)
    query_pos = query_tile * QUERY_TILE + lax.broadcasted_iota(
        jnp.int32, (KEY_TILE, QUERY_TILE), 1
    )
    return (key_pos <= query_pos) & (key_pos >= start_row)


def mm(left, right, left_dim=1, right_dim=0):
    return lax.dot_general(
        left, right, (((left_dim,), (right_dim,)), ((), ())), preferred_element_type=jnp.float32
    )


def pack_blocks(slot_ref, source_ref, target_ref, blocks):
    per_part = source_ref.shape[2] // BLOCK
    for block in range(blocks):
        slot = slot_ref[block]
        part = slot // per_part
        column = pl.multiple_of((slot % per_part) * BLOCK, BLOCK)
        target_ref[:, block * BLOCK : (block + 1) * BLOCK] = source_ref[
            part, :, pl.ds(column, BLOCK)
        ]


def attend_kernel(
    slot_ref, low_ref, qkv_ref, start_ref, out_ref, exact_ref, norm_ref, packed_ref, keys_ref
):
    total = packed_ref.shape[1]
    blocks = total // BLOCK
    pack_blocks(slot_ref, qkv_ref, packed_ref, blocks)
    for tile in range(total // KEY_TILE):
        spot = slice(tile * KEY_TILE, (tile + 1) * KEY_TILE)
        keys_ref[spot, :] = packed_ref[HD : 2 * HD, spot].T

    def query_step(query_tile, unused):
        column = pl.multiple_of(query_tile * QUERY_TILE, QUERY_TILE)
        queries = packed_ref[0:HD, pl.ds(column, QUERY_TILE)] * HD ** (-0.5)
        queries = queries.astype(jnp.bfloat16)
        start_row = start_ref[:, pl.ds(column, QUERY_TILE)]

        def key_step(key_tile, state):
            run_max, run_sum, run_out = state
            row = pl.multiple_of(key_tile * KEY_TILE, KEY_TILE)
            scores = mm(keys_ref[pl.ds(row, KEY_TILE), :], queries)
            scores = jnp.where(tile_mask(key_tile, query_tile, start_row), scores, MASKED)
            new_max = jnp.maximum(run_max, jnp.max(scores, axis=0, keepdims=True))
            probs = jnp.exp(scores - new_max)
            fade = jnp.exp(run_max - new_max)
            run_sum = run_sum * fade + jnp.sum(probs, axis=0, keepdims=True)
            run_out = run_out * fade + mm(
                packed_ref[2 * HD : 3 * HD, pl.ds(row, KEY_TILE)], probs.astype(jnp.bfloat16)
            )
            return new_max, run_sum, run_out

        first = (
            jnp.full((1, QUERY_TILE), -3e38, jnp.float32),
            jnp.zeros((1, QUERY_TILE), jnp.float32),
            jnp.zeros((HD, QUERY_TILE), jnp.float32),
        )
        run_max, run_sum, run_out = lax.fori_loop(
            low_ref[query_tile], ((query_tile + 1) * QUERY_TILE) // KEY_TILE, key_step, first
        )
        exact_ref[:, pl.ds(column, QUERY_TILE)] = run_out / run_sum
        norm_ref[:, pl.ds(column, QUERY_TILE)] = run_max + jnp.log(run_sum)
        return unused

    lax.fori_loop(0, total // QUERY_TILE, query_step, 0)
    per_part = out_ref.shape[2] // BLOCK
    for block in range(blocks):
        slot = slot_ref[block]
        column = pl.multiple_of((slot % per_part) * BLOCK, BLOCK)
        out_ref[slot // per_part, :, pl.ds(column, BLOCK)] = exact_ref[
            :, block * BLOCK : (block + 1) * BLOCK
        ].astype(jnp.bfloat16)


def rotate_back(values, cosine, sine_table):
    half_rot = ROT // 2
    lead_part = values[0:half_rot]
    tail_part = values[half_rot:ROT]
    return jnp.concatenate(
        [
            lead_part * cosine + tail_part * sine_table,
            tail_part * cosine - lead_part * sine_table,
            values[ROT:],
        ],
        axis=0,
    )


def attend_back_kernel(
    slot_ref,
    low_ref,
    grad_ref,
    packed_ref,
    exact_ref,
    norm_ref,
    start_ref,
    cosine_ref,
    sine_ref,
    out_ref,
    bias_ref,
    keys_ref,
    values_ref,
    grads_ref,
    sums_ref,
):
    total = packed_ref.shape[1]
    blocks = total // BLOCK
    scale = HD ** (-0.5)
    pack_blocks(slot_ref, grad_ref, grads_ref, blocks)
    for tile in range(total // KEY_TILE):
        spot = slice(tile * KEY_TILE, (tile + 1) * KEY_TILE)
        keys_ref[spot, :] = packed_ref[HD : 2 * HD, spot].T
        values_ref[spot, :] = packed_ref[2 * HD : 3 * HD, spot].T
    sums_ref[HD : 3 * HD, :] = jnp.zeros((2 * HD, total), jnp.float32)

    def query_step(query_tile, unused):
        column = pl.multiple_of(query_tile * QUERY_TILE, QUERY_TILE)
        spot = pl.ds(column, QUERY_TILE)
        queries = (packed_ref[0:HD, spot] * scale).astype(jnp.bfloat16)
        grads = grads_ref[:, spot]
        start_row = start_ref[:, spot]
        norm_row = norm_ref[:, spot]
        delta_row = jnp.sum(
            grads.astype(jnp.float32) * exact_ref[:, spot], axis=0, keepdims=True
        )

        def key_step(key_tile, grad_query):
            row = pl.multiple_of(key_tile * KEY_TILE, KEY_TILE)
            rows = pl.ds(row, KEY_TILE)
            scores = mm(keys_ref[rows, :], queries)
            scores = jnp.where(tile_mask(key_tile, query_tile, start_row), scores, MASKED)
            probs = jnp.exp(scores - norm_row)
            grad_probs = mm(values_ref[rows, :], grads)
            grad_scores = (probs * (grad_probs - delta_row)).astype(jnp.bfloat16)
            probs_b = probs.astype(jnp.bfloat16)
            sums_ref[2 * HD : 3 * HD, rows] += mm(grads, probs_b, 1, 1)
            sums_ref[HD : 2 * HD, rows] += mm(queries, grad_scores, 1, 1)
            return grad_query + mm(packed_ref[HD : 2 * HD, rows], grad_scores)

        grad_query = lax.fori_loop(
            low_ref[query_tile],
            ((query_tile + 1) * QUERY_TILE) // KEY_TILE,
            key_step,
            jnp.zeros((HD, QUERY_TILE), jnp.float32),
        )
        sums_ref[0:HD, spot] = grad_query * scale
        return unused

    lax.fori_loop(0, total // QUERY_TILE, query_step, 0)
    per_part = out_ref.shape[2] // BLOCK
    bias_sum = jnp.zeros((3 * HD, BLOCK), jnp.float32)
    for block in range(blocks):
        spot = slice(block * BLOCK, (block + 1) * BLOCK)
        cosine = cosine_ref[:, spot]
        sine_table = sine_ref[:, spot]
        slot = slot_ref[block]
        column = pl.multiple_of((slot % per_part) * BLOCK, BLOCK)
        rounded = jnp.concatenate(
            [
                rotate_back(sums_ref[0:HD, spot], cosine, sine_table),
                rotate_back(sums_ref[HD : 2 * HD, spot], cosine, sine_table),
                sums_ref[2 * HD : 3 * HD, spot],
            ],
            axis=0,
        ).astype(jnp.bfloat16)
        out_ref[slot // per_part, :, pl.ds(column, BLOCK)] = rounded
        bias_sum = bias_sum + rounded.astype(jnp.float32)
    bias_ref[...] = bias_sum


def attend_heads(slot_of, low_tile, qkv_parts, start_row):
    parts, _, part_rows = qkv_parts.shape
    total = parts * part_rows
    vmem = pl.BlockSpec(memory_space=pltpu.VMEM)
    return pl.pallas_call(
        attend_kernel,
        grid_spec=pltpu.PrefetchScalarGridSpec(
            num_scalar_prefetch=2,
            grid=(1,),
            in_specs=[vmem, vmem],
            out_specs=[vmem, vmem, vmem, vmem],
            scratch_shapes=[pltpu.VMEM((total, HD), jnp.bfloat16)],
        ),
        out_shape=[
            jax.ShapeDtypeStruct((parts, HD, part_rows), jnp.bfloat16),
            jax.ShapeDtypeStruct((HD, total), jnp.float32),
            jax.ShapeDtypeStruct((1, total), jnp.float32),
            jax.ShapeDtypeStruct((3 * HD, total), jnp.bfloat16),
        ],
        cost_estimate=pl.CostEstimate(
            flops=total * total * HD, transcendentals=total * total // 4, bytes_accessed=6 << 20
        ),
        compiler_params=pltpu.CompilerParams(vmem_limit_bytes=40 << 20),
        name="attend",
    )(slot_of, low_tile, qkv_parts, start_row)


def attend_heads_back(
    slot_of, low_tile, grad_parts, packed, exact, log_norm, start_row, cosine, sine_table
):
    parts, _, part_rows = grad_parts.shape
    total = parts * part_rows
    vmem = pl.BlockSpec(memory_space=pltpu.VMEM)
    return pl.pallas_call(
        attend_back_kernel,
        grid_spec=pltpu.PrefetchScalarGridSpec(
            num_scalar_prefetch=2,
            grid=(1,),
            in_specs=[vmem] * 7,
            out_specs=[vmem, vmem],
            scratch_shapes=[
                pltpu.VMEM((total, HD), jnp.bfloat16),
                pltpu.VMEM((total, HD), jnp.bfloat16),
                pltpu.VMEM((HD, total), jnp.bfloat16),
                pltpu.VMEM((3 * HD, total), jnp.float32),
            ],
        ),
        out_shape=[
            jax.ShapeDtypeStruct((parts, 3 * HD, part_rows), jnp.bfloat16),
            jax.ShapeDtypeStruct((3 * HD, BLOCK), jnp.float32),
        ],
        cost_estimate=pl.CostEstimate(
            flops=3 * total * total * HD,
            transcendentals=total * total // 4,
            bytes_accessed=8 << 20,
        ),
        compiler_params=pltpu.CompilerParams(vmem_limit_bytes=50 << 20),
        name="attend_back",
    )(slot_of, low_tile, grad_parts, packed, exact, log_norm, start_row, cosine, sine_table)


def start_of(position, seq_lengths):
    seq_ends = jnp.cumsum(seq_lengths)
    ends_before = seq_ends[:, None] <= position[None, :]
    return jnp.sum(jnp.where(ends_before, seq_lengths[:, None], 0), axis=0)


def rotary_tables(offset_in_seq):
    half_rot = ROT // 2
    freq_table = jnp.power(10000.0, -2.0 * jnp.arange(half_rot, dtype=jnp.float32) / ROT)
    angles = freq_table[:, None] * offset_in_seq.astype(jnp.float32)[None, :]
    return jnp.cos(angles), jnp.sin(angles)


def on_device_layer(*arrays):
    return on_device_heads(*arrays)


def on_device_heads(
    tokens,
    norm1_gain,
    norm1_bias,
    w_qkv,
    qkv_bias,
    w_out,
    norm2_gain,
    norm2_bias,
    w_gate,
    w_up,
    w_down,
    cotangent,
    seq_lengths,
    block_order,
):
    head_index = lax.axis_index("head")
    blk_index = lax.axis_index("blk")
    x_index, core_index = head_index // 2, head_index % 2
    z_index, y_index = blk_index // 2, blk_index % 2
    tok_rows, model_width = tokens.shape
    plane_rows = 8 * tok_rows
    total_rows = Z_PARTS * plane_rows
    row_block = model_width // (2 * Z_PARTS)
    chunk = 2 * row_block
    ff_half = w_gate.shape[1] // 2
    heads_width = Z_PARTS * HD

    qkv_split = w_qkv.reshape(row_block, 3, Z_PARTS, 2, HD)
    qkv_low = qkv_split[:, :, :, 0].reshape(row_block, 3 * heads_width)
    qkv_high = qkv_split[:, :, :, 1].reshape(row_block, 3 * heads_width)
    first = y_index == 0
    qkv_even, qkv_odd = to_even_odd(
        jnp.where(first, qkv_low, qkv_high), jnp.where(first, qkv_high, qkv_low), y_index
    )
    out_split = w_out.reshape(Z_PARTS, 2, HD, row_block)
    out_low = out_split[:, 0].reshape(heads_width, row_block)
    out_high = out_split[:, 1].reshape(heads_width, row_block)
    out_even, out_odd = to_even_odd(
        jnp.where(first, out_low, out_high), jnp.where(first, out_high, out_low), y_index
    )

    def column_halves(weight):
        low, high = weight[:, :ff_half], weight[:, ff_half:]
        return to_even_odd(jnp.where(first, low, high), jnp.where(first, high, low), y_index)

    gate_own = jnp.concatenate(column_halves(w_gate), axis=0)
    up_own = jnp.concatenate(column_halves(w_up), axis=0)
    down_low, down_high = w_down[:ff_half], w_down[ff_half:]
    down_even, down_odd = to_even_odd(
        jnp.where(first, down_low, down_high), jnp.where(first, down_high, down_low), y_index
    )

    def both_ways(even, odd, axis):
        forward = ring_gather(even, 1)
        backward = ring_gather(odd, -1)
        pieces = [p for pair in zip(forward, backward) for p in pair]
        return jnp.concatenate(pieces, axis=axis)

    x_own = split_order(tokens, z_index, 1).astype(jnp.float32)
    gain_one = split_order(norm1_gain, z_index, 0)
    shift_one = split_order(norm1_bias, z_index, 0)
    gain_two = split_order(norm2_gain, z_index, 0)
    shift_two = split_order(norm2_bias, z_index, 0)
    norm1_out, unit_one, inv_one = normalize(x_own, gain_one, shift_one)
    norm1_all = gather_rows(norm1_out.astype(jnp.bfloat16))
    qkv_full = both_ways(qkv_even, qkv_odd, 0)
    out_full = both_ways(out_even, out_odd, 1)
    gate_full = jnp.concatenate(ring_gather(gate_own, 1), axis=0)
    up_full = jnp.concatenate(ring_gather(up_own, -1), axis=0)
    down_full = both_ways(down_even, down_odd, 1)

    slots = jnp.arange(Z_PARTS * 8, dtype=jnp.int32)
    step_z, flip = slots // 8, slots % 8
    owner = (
        ((x_index ^ ((flip // 2) % 2)) * 2 + (core_index ^ (flip // 4))) * (2 * Z_PARTS)
        + ((z_index - step_z + Z_PARTS) % Z_PARTS) * 2
        + (y_index ^ (flip % 2))
    )
    packed_block = jnp.sum(
        jnp.where(owner[:, None] == slots[None, :], block_order[None, :], 0), axis=1
    )
    slot_of = jnp.sum(
        jnp.where(packed_block[None, :] == slots[:, None], slots[None, :], 0), axis=1
    )
    plane_pos = (
        packed_block[:8, None] * BLOCK + jnp.arange(BLOCK, dtype=jnp.int32)[None, :]
    ).reshape(-1)
    plane_cos, plane_sin = rotary_tables(plane_pos - start_of(plane_pos, seq_lengths))
    all_pos = jnp.arange(total_rows, dtype=jnp.int32)
    all_start = start_of(all_pos, seq_lengths)
    all_cos, all_sin = rotary_tables(all_pos - all_start)
    low_tile = (
        start_of(
            jnp.arange(total_rows // QUERY_TILE, dtype=jnp.int32) * QUERY_TILE, seq_lengths
        )
        // KEY_TILE
    )
    start_row = all_start[None, :]

    bias_split = qkv_bias.reshape(3, Z_PARTS, 2, HD)
    bias_own = jnp.where(first, bias_split[:, :, 0], bias_split[:, :, 1]).reshape(-1)
    projected = (mm(qkv_full, norm1_all, 0, 1) + bias_own[:, None]).reshape(
        3, Z_PARTS, HD, plane_rows
    )
    half_rot = ROT // 2
    lead_part, tail_part = projected[:2, :, :half_rot], projected[:2, :, half_rot:ROT]
    rotated = jnp.concatenate(
        [
            lead_part * plane_cos - tail_part * plane_sin,
            tail_part * plane_cos + lead_part * plane_sin,
            projected[:2, :, ROT:],
        ],
        axis=2,
    )
    qkv_heads = jnp.concatenate([rotated, projected[2:]], axis=0).astype(jnp.bfloat16)
    qkv_heads = qkv_heads.transpose(1, 0, 2, 3).reshape(Z_PARTS, 3 * HD, plane_rows)
    qkv_parts = to_heads(qkv_heads, z_index)
    attn_parts, attn_exact, log_norm, packed = attend_heads(
        slot_of, low_tile, qkv_parts, start_row
    )
    attn_t = from_heads(attn_parts, z_index).reshape(heads_width, plane_rows)
    attn_own = scatter_rows(mm(attn_t, out_full, 0, 0))

    hidden = x_own + attn_own
    norm2_out, unit_two, inv_two = normalize(hidden, gain_two, shift_two)
    norm2_all = gather_rows(norm2_out.astype(jnp.bfloat16))
    cotangent_own = split_order(cotangent, z_index, 1)
    grad_all = gather_rows(cotangent_own)
    gate_val = mm(norm2_all, gate_full)
    up_val = mm(norm2_all, up_full)
    sigmoid_gate = jax.nn.sigmoid(gate_val)
    swish_val = gate_val * sigmoid_gate
    activ_b = (swish_val * up_val).astype(jnp.bfloat16)
    grad_activ = mm(grad_all, down_full, 1, 1)
    grad_up_b = (grad_activ * swish_val).astype(jnp.bfloat16)
    grad_gate_b = (
        grad_activ * up_val * sigmoid_gate * (1.0 + gate_val * (1.0 - sigmoid_gate))
    ).astype(jnp.bfloat16)
    grad_norm2 = scatter_rows(mm(grad_gate_b, gate_full, 1, 1) + mm(grad_up_b, up_full, 1, 1))
    mlp_own = scatter_rows(mm(activ_b, down_full))
    output = split_order((hidden + mlp_own).astype(jnp.bfloat16), z_index, 1)

    def pieces_of(values, width, offset=0, size=None):
        size = width if size is None else size
        return [
            values[:, j * width + offset : j * width + offset + size] for j in range(Z_PARTS)
        ]

    down_sum_even = ring_scatter(
        [mm(activ_b, p, 0, 0) for p in pieces_of(grad_all, chunk, 0, row_block)], 1
    )
    down_sum_odd = ring_scatter(
        [mm(activ_b, p, 0, 0) for p in pieces_of(grad_all, chunk, row_block, row_block)], -1
    )
    down_parts = from_even_odd(down_sum_even, down_sum_odd, y_index)
    down_grad = jnp.concatenate(down_parts, axis=0)
    gate_sum = ring_scatter([mm(p, grad_gate_b, 0, 0) for p in pieces_of(norm2_all, chunk)], 1)
    up_sum = ring_scatter([mm(p, grad_up_b, 0, 0) for p in pieces_of(norm2_all, chunk)], -1)
    gate_grad = jnp.concatenate(
        from_even_odd(gate_sum[:row_block], gate_sum[row_block:], y_index), axis=1
    )
    up_grad = jnp.concatenate(
        from_even_odd(up_sum[:row_block], up_sum[row_block:], y_index), axis=1
    )

    grad_out = cotangent_own.astype(jnp.float32)
    grad_hidden = grad_out + normalize_back(grad_norm2, unit_two, inv_two, gain_two)
    branch_all = gather_rows(grad_hidden.astype(jnp.bfloat16))
    grad_attn = (
        mm(out_full, branch_all, 1, 1)
        .astype(jnp.bfloat16)
        .reshape(Z_PARTS, HD, plane_rows)
    )
    grad_parts = to_heads(grad_attn, z_index)
    proj_parts, bias_sums = attend_heads_back(
        slot_of, low_tile, grad_parts, packed, attn_exact, log_norm, start_row, all_cos, all_sin
    )
    bias_grad = jnp.sum(bias_sums, axis=1).reshape(3, HD)
    grad_proj = from_heads(proj_parts, z_index).reshape(Z_PARTS, 3, HD, plane_rows)
    grad_proj = grad_proj.transpose(1, 0, 2, 3).reshape(3 * heads_width, plane_rows)
    grad_norm1 = scatter_rows(mm(grad_proj, qkv_full, 0, 1))

    out_sum_even = ring_scatter(
        [mm(attn_t, p) for p in pieces_of(branch_all, chunk, 0, row_block)], 1
    )
    out_sum_odd = ring_scatter(
        [mm(attn_t, p) for p in pieces_of(branch_all, chunk, row_block, row_block)], -1
    )
    out_parts = from_even_odd(out_sum_even, out_sum_odd, y_index)
    out_grad = jnp.stack(
        [p.reshape(Z_PARTS, HD, row_block) for p in out_parts], axis=1
    ).reshape(w_out.shape)
    qkv_sum_even = ring_scatter(
        [mm(p, grad_proj, 0, 1) for p in pieces_of(norm1_all, chunk, 0, row_block)], 1
    )
    qkv_sum_odd = ring_scatter(
        [mm(p, grad_proj, 0, 1) for p in pieces_of(norm1_all, chunk, row_block, row_block)], -1
    )
    qkv_grad_parts = from_even_odd(qkv_sum_even, qkv_sum_odd, y_index)
    qkv_grad = jnp.stack(
        [p.reshape(row_block, 3, Z_PARTS, HD) for p in qkv_grad_parts], axis=3
    ).reshape(w_qkv.shape)

    input_grad = grad_hidden + normalize_back(grad_norm1, unit_one, inv_one, gain_one)
    sums = jnp.stack(
        [
            jnp.sum(grad_norm1 * unit_one, axis=0),
            jnp.sum(grad_norm1, axis=0),
            jnp.sum(grad_norm2 * unit_two, axis=0),
            jnp.sum(grad_norm2, axis=0),
        ],
        axis=0,
    )
    norm_sums = scatter_sums(
        split_order(sums, z_index, 1), x_index, core_index, z_index, y_index
    )
    return (
        output,
        split_order(input_grad, z_index, 1),
        norm_sums[0],
        norm_sums[1],
        qkv_grad,
        bias_grad,
        out_grad,
        norm_sums[2],
        norm_sums[3],
        gate_grad,
        up_grad,
        down_grad,
    )


def solution(mesh):
    placed = (
        P(("head", "blk"), None),
        P(),
        P(),
        P("blk", None, "head"),
        P(None, "head"),
        P("head", "blk"),
        P(),
        P(),
        P("blk", "head"),
        P("blk", "head"),
        P("head", "blk"),
        P(("head", "blk"), None),
        P(),
        P(),
    )
    heads_plan = mesh.shape["head"] == 4 and mesh.shape["blk"] == 2 * Z_PARTS
    return jax.shard_map(
        on_device_layer if heads_plan else on_device,
        mesh=mesh,
        in_specs=placed,
        out_specs=(
            P(("head", "blk"), None),
            P(("head", "blk"), None),
            P(("head", "blk")),
            P(("head", "blk")),
            P("blk", None, "head"),
            P(None, ("head", "blk")),
            P("head", "blk"),
            P(("head", "blk")),
            P(("head", "blk")),
            P("blk", "head"),
            P("blk", "head"),
            P("head", "blk"),
        ),
        check_vma=False,
    )
```

```python
import jax
import jax.numpy as jnp
from jax import lax
from jax.experimental import pallas as pl
from jax.experimental.pallas import tpu as pltpu
from jax.sharding import PartitionSpec as P


HD = 64
ROT = 16
BLOCK = 128
Z_PARTS = 4
QUERY_TILE = 512
KEY_TILE = 256


EPSILON = 1e-05
MASKED = -1000000000.0


def contract_rows(left, right):
    return lax.dot_general(
        left, right, (((0,), (0,)), ((), ())), preferred_element_type=jnp.float32
    )


def times_transpose(left, right):
    return lax.dot_general(
        left, right, (((1,), (1,)), ((), ())), preferred_element_type=jnp.float32
    )


def packed_positions(row_ids, block_order):
    block_ids = jnp.arange(block_order.shape[0], dtype=jnp.int32)
    matches = (row_ids // BLOCK)[:, None] == block_ids[None, :]
    block_start = jnp.sum(jnp.where(matches, block_order[None, :], 0), axis=1)
    return block_start * BLOCK + row_ids % BLOCK


def sequence_start(position, seq_lengths):
    seq_ends = jnp.cumsum(seq_lengths)
    ends_before = seq_ends[None, :] <= position[:, None]
    return jnp.sum(jnp.where(ends_before, seq_lengths[None, :], 0), axis=1)


def rotate(values, cosine, sine_table):
    half_rot = ROT // 2
    lead_part = values[..., :half_rot]
    tail_part = values[..., half_rot:ROT]
    cos_rows = cosine[:, None, :]
    sin_rows = sine_table[:, None, :]
    return jnp.concatenate(
        [
            lead_part * cos_rows - tail_part * sin_rows,
            tail_part * cos_rows + lead_part * sin_rows,
            values[..., ROT:],
        ],
        axis=-1,
    )


def normalize(values, norm_gain, norm_shift):
    centre = values - jnp.mean(values, axis=-1, keepdims=True)
    inv_scale = lax.rsqrt(jnp.mean(centre * centre, axis=-1, keepdims=True) + EPSILON)
    unit_rows = centre * inv_scale
    return (unit_rows * norm_gain + norm_shift, unit_rows, inv_scale)


def normalize_back(grad_norm, unit_rows, inv_scale, norm_gain):
    grad_unit = grad_norm * norm_gain
    mean_grad = jnp.mean(grad_unit, axis=-1, keepdims=True)
    mean_proj = jnp.mean(grad_unit * unit_rows, axis=-1, keepdims=True)
    return inv_scale * (grad_unit - mean_grad - unit_rows * mean_proj)


def gather_keys(keys_flat, values_flat):
    return (
        lax.all_gather(keys_flat, "blk", axis=0, tiled=True),
        lax.all_gather(values_flat, "blk", axis=0, tiled=True),
    )


def tile_count_of(total_rows):
    tile_rows = min(1024, total_rows)
    return (total_rows // tile_rows, tile_rows)


def key_tiles(keys_all, values_all, key_pos, heads_local):
    tile_count, tile_rows = tile_count_of(keys_all.shape[0])
    return (
        keys_all.reshape(tile_count, tile_rows, heads_local, HD),
        values_all.reshape(tile_count, tile_rows, heads_local, HD),
        key_pos.reshape(tile_count, tile_rows),
    )


def masked_scores(queries, key_tile, pos_tile, query_pos, query_start):
    raw_scores = jnp.einsum(
        "qhd,khd->hqk", queries, key_tile, preferred_element_type=jnp.float32
    ) * HD ** (-0.5)
    allowed = (pos_tile[None, :] <= query_pos[:, None]) & (
        pos_tile[None, :] >= query_start[:, None]
    )
    return jnp.where(allowed[None], raw_scores, MASKED)


def attend(queries, tiles, query_pos, query_start):
    group_rows = queries.shape[0]
    heads_local = queries.shape[1]

    def first_pass(run_state, tile):
        run_max, run_sum = run_state
        scores = masked_scores(queries, tile[0], tile[2], query_pos, query_start)
        new_max = jnp.maximum(run_max, jnp.max(scores, axis=-1))
        new_sum = run_sum * jnp.exp(run_max - new_max) + jnp.sum(
            jnp.exp(scores - new_max[..., None]), axis=-1
        )
        return ((new_max, new_sum), None)

    start_state = (
        jnp.full((heads_local, group_rows), -3e38, jnp.float32),
        jnp.zeros((heads_local, group_rows), jnp.float32),
    )
    (run_max, run_sum), unused = lax.scan(first_pass, start_state, tiles)
    log_norm = run_max + jnp.log(run_sum)

    def second_pass(totals, tile):
        total_out, total_rest = totals
        scores = masked_scores(queries, tile[0], tile[2], query_pos, query_start)
        probs_f32 = jnp.exp(scores - log_norm[..., None])
        probs_b = probs_f32.astype(jnp.bfloat16)
        rest_b = (probs_f32 - probs_b.astype(jnp.float32)).astype(jnp.bfloat16)
        total_out = total_out + jnp.einsum(
            "hqk,khd->qhd", probs_b, tile[1], preferred_element_type=jnp.float32
        )
        total_rest = total_rest + jnp.einsum(
            "hqk,khd->qhd", rest_b, tile[1], preferred_element_type=jnp.float32
        )
        return ((total_out, total_rest), None)

    empty = jnp.zeros((group_rows, heads_local, HD), jnp.float32)
    (attended, leftover), unused = lax.scan(second_pass, (empty, empty), tiles)
    return (attended, attended + leftover, log_norm)


def attend_back(queries, tiles, query_pos, query_start, log_norm, grad_attn, delta_rows):
    scale = HD ** (-0.5)

    def step_back(grad_query, tile):
        key_tile, value_tile, pos_tile = tile
        scores = masked_scores(queries, key_tile, pos_tile, query_pos, query_start)
        probs_f32 = jnp.exp(scores - log_norm[..., None])
        grad_probs = jnp.einsum(
            "qhd,khd->hqk", grad_attn, value_tile, preferred_element_type=jnp.float32
        )
        grad_scores = (probs_f32 * (grad_probs - delta_rows[..., None])).astype(jnp.bfloat16)
        probs_b = probs_f32.astype(jnp.bfloat16)
        grad_query = grad_query + scale * jnp.einsum(
            "hqk,khd->qhd", grad_scores, key_tile, preferred_element_type=jnp.float32
        )
        grad_key = scale * jnp.einsum(
            "hqk,qhd->khd", grad_scores, queries, preferred_element_type=jnp.float32
        )
        grad_value = jnp.einsum(
            "hqk,qhd->khd", probs_b, grad_attn, preferred_element_type=jnp.float32
        )
        return (grad_query, (grad_key, grad_value))

    grad_query, (grad_keys, grad_values) = lax.scan(
        step_back, jnp.zeros(queries.shape, jnp.float32), tiles
    )
    return (grad_query, grad_keys, grad_values)


def on_device(
    tokens,
    norm1_gain,
    norm1_bias,
    w_qkv,
    qkv_bias,
    w_out,
    norm2_gain,
    norm2_bias,
    w_gate,
    w_up,
    w_down,
    cotangent,
    seq_lengths,
    block_order,
):
    team_count = lax.axis_size("head")
    span_count = lax.axis_size("blk")
    span_index = lax.axis_index("blk")
    tok_rows = tokens.shape[0]
    model_width = tokens.shape[1]
    group_rows = tok_rows * team_count
    local_width = w_out.shape[0]
    heads_local = local_width // HD
    offsets = jnp.arange(tok_rows, dtype=jnp.int32)
    member = jnp.arange(team_count, dtype=jnp.int32)
    owner_index = jnp.arange(span_count, dtype=jnp.int32)
    query_ids = ((member[:, None] * span_count + span_index) * tok_rows + offsets[None, :]).reshape(
        -1
    )
    key_ids = (
        (member[None, :, None] * span_count + owner_index[:, None, None]) * tok_rows
        + offsets[None, None, :]
    ).reshape(-1)
    query_pos = packed_positions(query_ids, block_order)
    query_start = sequence_start(query_pos, seq_lengths)
    key_pos = packed_positions(key_ids, block_order)
    half_rot = ROT // 2
    freq_table = jnp.power(10000.0, -2.0 * jnp.arange(half_rot, dtype=jnp.float32) / ROT)
    angles = (query_pos - query_start).astype(jnp.float32)[:, None] * freq_table[None, :]
    cosine = jnp.cos(angles)
    sine_table = jnp.sin(angles)
    x_own = tokens.astype(jnp.float32)
    norm1_out, unit_one, inv_one = normalize(x_own, norm1_gain, norm1_bias)
    norm1_group = lax.all_gather(norm1_out.astype(jnp.bfloat16), "head", axis=0, tiled=True)
    qkv_full, out_full = (
        lax.all_gather(w_qkv, "blk", axis=0, tiled=True),
        lax.all_gather(w_out, "blk", axis=1, tiled=True),
    )
    qkv_matrix = qkv_full.reshape(model_width, 3 * local_width)
    projected = jnp.dot(
        norm1_group, qkv_matrix, preferred_element_type=jnp.float32
    ) + qkv_bias.reshape(1, -1)
    projected = projected.reshape(group_rows, 3, heads_local, HD)
    queries = rotate(projected[:, 0], cosine, sine_table).astype(jnp.bfloat16)
    keys_flat = (
        rotate(projected[:, 1], cosine, sine_table)
        .astype(jnp.bfloat16)
        .reshape(group_rows, local_width)
    )
    values_flat = projected[:, 2].astype(jnp.bfloat16).reshape(group_rows, local_width)
    keys_all, values_all = gather_keys(keys_flat, values_flat)
    attn_out, attn_exact, log_norm = attend(
        queries, key_tiles(keys_all, values_all, key_pos, heads_local), query_pos, query_start
    )
    attn_b = attn_out.reshape(group_rows, local_width).astype(jnp.bfloat16)
    attn_own = lax.psum_scatter(
        jnp.dot(attn_b, out_full, preferred_element_type=jnp.float32),
        "head",
        scatter_dimension=0,
        tiled=True,
    )
    hidden = x_own + attn_own
    norm2_out, unit_two, inv_two = normalize(hidden, norm2_gain, norm2_bias)
    norm2_group = lax.all_gather(norm2_out.astype(jnp.bfloat16), "head", axis=0, tiled=True)
    gate_full, up_full, down_full = (
        lax.all_gather(w_gate, "blk", axis=0, tiled=True),
        lax.all_gather(w_up, "blk", axis=0, tiled=True),
        lax.all_gather(w_down, "blk", axis=1, tiled=True),
    )
    gate_val = jnp.dot(norm2_group, gate_full, preferred_element_type=jnp.float32)
    up_val = jnp.dot(norm2_group, up_full, preferred_element_type=jnp.float32)
    sigmoid_gate = jax.nn.sigmoid(gate_val)
    swish_val = gate_val * sigmoid_gate
    activ_b = (swish_val * up_val).astype(jnp.bfloat16)
    mlp_own = lax.psum_scatter(
        jnp.dot(activ_b, down_full, preferred_element_type=jnp.float32).astype(jnp.bfloat16),
        "head",
        scatter_dimension=0,
        tiled=True,
    ).astype(jnp.float32)
    output = (hidden + mlp_own).astype(jnp.bfloat16)
    grad_out = cotangent.astype(jnp.float32)
    grad_group = lax.all_gather(cotangent, "head", axis=0, tiled=True)
    grad_activ = times_transpose(grad_group, down_full)
    grad_w_down = contract_rows(activ_b, grad_group)
    grad_up_b = (grad_activ * swish_val).astype(jnp.bfloat16)
    grad_gate_b = (
        grad_activ * up_val * sigmoid_gate * (1.0 + gate_val * (1.0 - sigmoid_gate))
    ).astype(jnp.bfloat16)
    grad_w_gate = contract_rows(norm2_group, grad_gate_b)
    grad_w_up = contract_rows(norm2_group, grad_up_b)
    grad_norm2 = lax.psum_scatter(
        times_transpose(grad_gate_b, gate_full) + times_transpose(grad_up_b, up_full),
        "head",
        scatter_dimension=0,
        tiled=True,
    )
    grad_hidden = grad_out + normalize_back(grad_norm2, unit_two, inv_two, norm2_gain)
    gain_two_grad = jnp.sum(grad_norm2 * unit_two, axis=0)
    shift_two_grad = jnp.sum(grad_norm2, axis=0)
    branch_group = lax.all_gather(grad_hidden.astype(jnp.bfloat16), "head", axis=0, tiled=True)
    grad_w_out = contract_rows(attn_b, branch_group)
    grad_attn = (
        times_transpose(branch_group, out_full)
        .astype(jnp.bfloat16)
        .reshape(group_rows, heads_local, HD)
    )
    delta_rows = jnp.sum(grad_attn.astype(jnp.float32) * attn_exact, axis=-1).T
    keys_back_all, values_back_all = gather_keys(keys_flat, values_flat)
    tiles_back = key_tiles(keys_back_all, values_back_all, key_pos, heads_local)
    grad_query, grad_keys, grad_values = attend_back(
        queries, tiles_back, query_pos, query_start, log_norm, grad_attn, delta_rows
    )
    key_terms = grad_keys.reshape(-1, local_width)
    value_terms = grad_values.reshape(-1, local_width)
    grad_key_own, grad_value_own = (
        lax.psum_scatter(
            key_terms.astype(jnp.bfloat16), "blk", scatter_dimension=0, tiled=True
        ).astype(jnp.float32),
        lax.psum_scatter(
            value_terms.astype(jnp.bfloat16), "blk", scatter_dimension=0, tiled=True
        ).astype(jnp.float32),
    )
    grad_query_pre = rotate(grad_query, cosine, -sine_table).reshape(group_rows, local_width)
    grad_key_pre = rotate(
        grad_key_own.reshape(group_rows, heads_local, HD), cosine, -sine_table
    ).reshape(group_rows, local_width)
    grad_proj_b = jnp.stack([grad_query_pre, grad_key_pre, grad_value_own], axis=1).astype(
        jnp.bfloat16
    )
    bias_grad = jnp.sum(grad_proj_b.astype(jnp.float32), axis=0)
    grad_proj_flat = grad_proj_b.reshape(group_rows, 3 * local_width)
    grad_w_qkv = contract_rows(norm1_group, grad_proj_flat).reshape(model_width, 3, local_width)
    grad_norm1 = lax.psum_scatter(
        times_transpose(grad_proj_flat, qkv_matrix).astype(jnp.bfloat16),
        "head",
        scatter_dimension=0,
        tiled=True,
    ).astype(jnp.float32)
    input_grad = grad_hidden + normalize_back(grad_norm1, unit_one, inv_one, norm1_gain)
    gain_one_grad = jnp.sum(grad_norm1 * unit_one, axis=0)
    shift_one_grad = jnp.sum(grad_norm1, axis=0)
    norm_sums = (
        lax.psum_scatter(gain_one_grad, ("head", "blk"), scatter_dimension=0, tiled=True),
        lax.psum_scatter(shift_one_grad, ("head", "blk"), scatter_dimension=0, tiled=True),
        lax.psum_scatter(gain_two_grad, ("head", "blk"), scatter_dimension=0, tiled=True),
        lax.psum_scatter(shift_two_grad, ("head", "blk"), scatter_dimension=0, tiled=True),
    )
    grad_shards = (
        lax.psum_scatter(
            grad_w_qkv.astype(jnp.bfloat16), "blk", scatter_dimension=0, tiled=True
        ).astype(jnp.float32),
        lax.psum_scatter(
            bias_grad.astype(jnp.bfloat16), "blk", scatter_dimension=1, tiled=True
        ).astype(jnp.float32),
        lax.psum_scatter(
            grad_w_out.astype(jnp.bfloat16), "blk", scatter_dimension=1, tiled=True
        ).astype(jnp.float32),
        lax.psum_scatter(
            grad_w_gate.astype(jnp.bfloat16), "blk", scatter_dimension=0, tiled=True
        ).astype(jnp.float32),
        lax.psum_scatter(
            grad_w_up.astype(jnp.bfloat16), "blk", scatter_dimension=0, tiled=True
        ).astype(jnp.float32),
        lax.psum_scatter(
            grad_w_down.astype(jnp.bfloat16), "blk", scatter_dimension=1, tiled=True
        ).astype(jnp.float32),
    )
    return (
        output,
        input_grad,
        norm_sums[0],
        norm_sums[1],
        grad_shards[0],
        grad_shards[1],
        grad_shards[2],
        norm_sums[2],
        norm_sums[3],
        grad_shards[3],
        grad_shards[4],
        grad_shards[5],
    )


def split_order(values, z_index, axis):
    pieces = values.shape[axis] // Z_PARTS
    parts = [
        lax.dynamic_slice_in_dim(
            values, lax.rem(z_index - j + Z_PARTS, Z_PARTS) * pieces, pieces, axis
        )
        for j in range(Z_PARTS)
    ]
    return jnp.concatenate(parts, axis=axis)


def swap_x(values):
    return lax.ppermute(values, "head", [(h, h ^ 2) for h in range(4)])


def swap_core(values):
    return lax.ppermute(values, "head", [(h, h ^ 1) for h in range(4)])


def swap_y(values):
    return lax.ppermute(values, "blk", [(b, b ^ 1) for b in range(2 * Z_PARTS)])


def shift_z(values, amount):
    total = 2 * Z_PARTS
    return lax.ppermute(values, "blk", [(b, (b + 2 * amount) % total) for b in range(total)])


def swap_low_z(values):
    return lax.ppermute(values, "blk", [(b, b ^ 2) for b in range(2 * Z_PARTS)])


def gather_rows(own):
    half = own.shape[0] // 2
    from_x = swap_x(own)
    from_y = swap_y(own)
    corner_a = swap_y(from_x[:half])
    corner_b = swap_x(from_y[half:])
    mine = jnp.concatenate([own, from_y, from_x, corner_a, corner_b], axis=0)
    other = swap_core(mine)
    return jnp.concatenate([mine, other], axis=0)


def scatter_rows(partial):
    rows = partial.shape[0] // 8
    half = rows // 2
    mine = partial[: 4 * rows]
    theirs = swap_core(partial[4 * rows :].astype(jnp.bfloat16))
    total = mine + theirs.astype(jnp.float32)
    own, for_y, for_x, corner = [total[i * rows : (i + 1) * rows] for i in range(4)]
    corner_b = corner.astype(jnp.bfloat16)
    got_x = swap_x(corner_b[:half]).astype(jnp.float32)
    got_y = swap_y(corner_b[half:]).astype(jnp.float32)
    for_y = jnp.concatenate([for_y[:half] + got_x, for_y[half:]], axis=0)
    for_x = jnp.concatenate([for_x[:half], for_x[half:] + got_y], axis=0)
    last_x = swap_x(for_x.astype(jnp.bfloat16)).astype(jnp.float32)
    last_y = swap_y(for_y.astype(jnp.bfloat16)).astype(jnp.float32)
    return own + last_x + last_y


def halve(values, bit, swap):
    mine = lax.dynamic_index_in_dim(values, bit, axis=0, keepdims=False)
    theirs = lax.dynamic_index_in_dim(values, 1 - bit, axis=0, keepdims=False)
    return mine + swap(theirs)


def scatter_sums(sums, x_index, core_index, z_index, y_index):
    count, width = sums.shape
    total = sums.reshape(count, 2, 2, 2, 2, 2, width // 32).transpose(1, 2, 3, 4, 5, 0, 6)
    total = halve(total, x_index, swap_x)
    total = halve(total, core_index, swap_core)
    total = halve(total, z_index // 2, lambda v: shift_z(v, 2))
    total = halve(total, z_index % 2, swap_low_z)
    return halve(total, y_index, swap_y)


def ring_gather(chunk, amount):
    held = [chunk]
    for _ in range(1, Z_PARTS):
        held.append(shift_z(held[-1], amount))
    if amount == 1:
        return held
    return [held[(Z_PARTS - j) % Z_PARTS] for j in range(Z_PARTS)]


def ring_scatter(partials, amount):
    order = [(j + 1) % Z_PARTS for j in range(Z_PARTS)]
    if amount == -1:
        order = [(Z_PARTS - j) % Z_PARTS for j in order]
    total = partials[order[0]]()
    sent = total.astype(jnp.bfloat16)
    for hop in range(1, Z_PARTS):
        moved = shift_z(sent, amount)
        total = moved.astype(jnp.float32) + partials[order[hop]]()
        sent = total.astype(jnp.bfloat16)
    return total


def to_even_odd(mine, theirs, y_index):
    got = swap_y(theirs)
    return jnp.where(y_index == 0, mine, got), jnp.where(y_index == 0, got, mine)


def from_even_odd(even, odd, y_index):
    mine = jnp.where(y_index == 0, even, odd)
    theirs = jnp.where(y_index == 0, odd, even).astype(jnp.bfloat16)
    got = swap_y(theirs).astype(jnp.float32)
    return jnp.where(y_index == 0, mine, got), jnp.where(y_index == 0, got, mine)


def to_heads(pieces, z_index):
    received = []
    for t in range(Z_PARTS):
        piece = lax.dynamic_index_in_dim(
            pieces, lax.rem(z_index + t, Z_PARTS), axis=0, keepdims=False
        )
        received.append(piece if t == 0 else shift_z(piece, t))
    return jnp.stack(received, axis=0)


def from_heads(pieces, z_index):
    received = [pieces[0]] + [shift_z(pieces[t], -t) for t in range(1, Z_PARTS)]
    ordered = jnp.stack(received + received, axis=0)
    return lax.dynamic_slice_in_dim(ordered, Z_PARTS - z_index, Z_PARTS, axis=0)


def tile_mask(key_tile, query_tile, start_row):
    key_pos = key_tile * KEY_TILE + lax.broadcasted_iota(jnp.int32, (KEY_TILE, QUERY_TILE), 0)
    query_pos = query_tile * QUERY_TILE + lax.broadcasted_iota(
        jnp.int32, (KEY_TILE, QUERY_TILE), 1
    )
    return (key_pos <= query_pos) & (key_pos >= start_row)


def mm(left, right, left_dim=1, right_dim=0):
    return lax.dot_general(
        left, right, (((left_dim,), (right_dim,)), ((), ())), preferred_element_type=jnp.float32
    )


def pack_blocks(slot_ref, source_ref, target_ref, blocks):
    per_part = source_ref.shape[2] // BLOCK
    for block in range(blocks):
        slot = slot_ref[block]
        part = slot // per_part
        column = pl.multiple_of((slot % per_part) * BLOCK, BLOCK)
        target_ref[:, block * BLOCK : (block + 1) * BLOCK] = source_ref[
            part, :, pl.ds(column, BLOCK)
        ]


def attend_kernel(
    slot_ref, low_ref, qkv_ref, start_ref, out_ref, exact_ref, norm_ref, packed_ref, keys_ref
):
    total = packed_ref.shape[1]
    blocks = total // BLOCK
    pack_blocks(slot_ref, qkv_ref, packed_ref, blocks)
    for tile in range(total // KEY_TILE):
        spot = slice(tile * KEY_TILE, (tile + 1) * KEY_TILE)
        keys_ref[spot, :] = packed_ref[HD : 2 * HD, spot].T

    def query_step(query_tile, unused):
        column = pl.multiple_of(query_tile * QUERY_TILE, QUERY_TILE)
        queries = packed_ref[0:HD, pl.ds(column, QUERY_TILE)] * HD ** (-0.5)
        queries = queries.astype(jnp.bfloat16)
        start_row = start_ref[:, pl.ds(column, QUERY_TILE)]

        def key_step(key_tile, state):
            run_max, run_sum, run_out = state
            row = pl.multiple_of(key_tile * KEY_TILE, KEY_TILE)
            scores = mm(keys_ref[pl.ds(row, KEY_TILE), :], queries)
            scores = jnp.where(tile_mask(key_tile, query_tile, start_row), scores, MASKED)
            new_max = jnp.maximum(run_max, jnp.max(scores, axis=0, keepdims=True))
            probs = jnp.exp(scores - new_max)
            fade = jnp.exp(run_max - new_max)
            run_sum = run_sum * fade + jnp.sum(probs, axis=0, keepdims=True)
            run_out = run_out * fade + mm(
                packed_ref[2 * HD : 3 * HD, pl.ds(row, KEY_TILE)], probs.astype(jnp.bfloat16)
            )
            return new_max, run_sum, run_out

        first = (
            jnp.full((1, QUERY_TILE), -3e38, jnp.float32),
            jnp.zeros((1, QUERY_TILE), jnp.float32),
            jnp.zeros((HD, QUERY_TILE), jnp.float32),
        )
        run_max, run_sum, run_out = lax.fori_loop(
            low_ref[query_tile], ((query_tile + 1) * QUERY_TILE) // KEY_TILE, key_step, first
        )
        exact_ref[:, pl.ds(column, QUERY_TILE)] = run_out / run_sum
        norm_ref[:, pl.ds(column, QUERY_TILE)] = run_max + jnp.log(run_sum)
        return unused

    lax.fori_loop(0, total // QUERY_TILE, query_step, 0)
    per_part = out_ref.shape[2] // BLOCK
    for block in range(blocks):
        slot = slot_ref[block]
        column = pl.multiple_of((slot % per_part) * BLOCK, BLOCK)
        out_ref[slot // per_part, :, pl.ds(column, BLOCK)] = exact_ref[
            :, block * BLOCK : (block + 1) * BLOCK
        ].astype(jnp.bfloat16)


def rotate_back(values, cosine, sine_table):
    half_rot = ROT // 2
    lead_part = values[0:half_rot]
    tail_part = values[half_rot:ROT]
    return jnp.concatenate(
        [
            lead_part * cosine + tail_part * sine_table,
            tail_part * cosine - lead_part * sine_table,
            values[ROT:],
        ],
        axis=0,
    )


def attend_back_kernel(
    slot_ref,
    low_ref,
    grad_ref,
    packed_ref,
    exact_ref,
    norm_ref,
    start_ref,
    cosine_ref,
    sine_ref,
    out_ref,
    bias_ref,
    keys_ref,
    values_ref,
    grads_ref,
    sums_ref,
):
    total = packed_ref.shape[1]
    blocks = total // BLOCK
    scale = HD ** (-0.5)
    pack_blocks(slot_ref, grad_ref, grads_ref, blocks)
    for tile in range(total // KEY_TILE):
        spot = slice(tile * KEY_TILE, (tile + 1) * KEY_TILE)
        keys_ref[spot, :] = packed_ref[HD : 2 * HD, spot].T
        values_ref[spot, :] = packed_ref[2 * HD : 3 * HD, spot].T
    sums_ref[HD : 3 * HD, :] = jnp.zeros((2 * HD, total), jnp.float32)

    def query_step(query_tile, unused):
        column = pl.multiple_of(query_tile * QUERY_TILE, QUERY_TILE)
        spot = pl.ds(column, QUERY_TILE)
        queries = (packed_ref[0:HD, spot] * scale).astype(jnp.bfloat16)
        grads = grads_ref[:, spot]
        start_row = start_ref[:, spot]
        norm_row = norm_ref[:, spot]
        delta_row = jnp.sum(
            grads.astype(jnp.float32) * exact_ref[:, spot], axis=0, keepdims=True
        )

        def key_step(key_tile, grad_query):
            row = pl.multiple_of(key_tile * KEY_TILE, KEY_TILE)
            rows = pl.ds(row, KEY_TILE)
            scores = mm(keys_ref[rows, :], queries)
            scores = jnp.where(tile_mask(key_tile, query_tile, start_row), scores, MASKED)
            probs = jnp.exp(scores - norm_row)
            grad_probs = mm(values_ref[rows, :], grads)
            grad_scores = (probs * (grad_probs - delta_row)).astype(jnp.bfloat16)
            probs_b = probs.astype(jnp.bfloat16)
            sums_ref[2 * HD : 3 * HD, rows] += mm(grads, probs_b, 1, 1)
            sums_ref[HD : 2 * HD, rows] += mm(queries, grad_scores, 1, 1)
            return grad_query + mm(packed_ref[HD : 2 * HD, rows], grad_scores)

        grad_query = lax.fori_loop(
            low_ref[query_tile],
            ((query_tile + 1) * QUERY_TILE) // KEY_TILE,
            key_step,
            jnp.zeros((HD, QUERY_TILE), jnp.float32),
        )
        sums_ref[0:HD, spot] = grad_query * scale
        return unused

    lax.fori_loop(0, total // QUERY_TILE, query_step, 0)
    per_part = out_ref.shape[2] // BLOCK
    bias_sum = jnp.zeros((3 * HD, BLOCK), jnp.float32)
    for block in range(blocks):
        spot = slice(block * BLOCK, (block + 1) * BLOCK)
        cosine = cosine_ref[:, spot]
        sine_table = sine_ref[:, spot]
        slot = slot_ref[block]
        column = pl.multiple_of((slot % per_part) * BLOCK, BLOCK)
        rounded = jnp.concatenate(
            [
                rotate_back(sums_ref[0:HD, spot], cosine, sine_table),
                rotate_back(sums_ref[HD : 2 * HD, spot], cosine, sine_table),
                sums_ref[2 * HD : 3 * HD, spot],
            ],
            axis=0,
        ).astype(jnp.bfloat16)
        out_ref[slot // per_part, :, pl.ds(column, BLOCK)] = rounded
        bias_sum = bias_sum + rounded.astype(jnp.float32)
    bias_ref[...] = bias_sum


def attend_heads(slot_of, low_tile, qkv_parts, start_row):
    parts, _, part_rows = qkv_parts.shape
    total = parts * part_rows
    vmem = pl.BlockSpec(memory_space=pltpu.VMEM)
    return pl.pallas_call(
        attend_kernel,
        grid_spec=pltpu.PrefetchScalarGridSpec(
            num_scalar_prefetch=2,
            grid=(1,),
            in_specs=[vmem, vmem],
            out_specs=[vmem, vmem, vmem, vmem],
            scratch_shapes=[pltpu.VMEM((total, HD), jnp.bfloat16)],
        ),
        out_shape=[
            jax.ShapeDtypeStruct((parts, HD, part_rows), jnp.bfloat16),
            jax.ShapeDtypeStruct((HD, total), jnp.float32),
            jax.ShapeDtypeStruct((1, total), jnp.float32),
            jax.ShapeDtypeStruct((3 * HD, total), jnp.bfloat16),
        ],
        cost_estimate=pl.CostEstimate(
            flops=total * total * HD, transcendentals=total * total // 4, bytes_accessed=6 << 20
        ),
        compiler_params=pltpu.CompilerParams(vmem_limit_bytes=40 << 20),
        name="attend",
    )(slot_of, low_tile, qkv_parts, start_row)


def attend_heads_back(
    slot_of, low_tile, grad_parts, packed, exact, log_norm, start_row, cosine, sine_table
):
    parts, _, part_rows = grad_parts.shape
    total = parts * part_rows
    vmem = pl.BlockSpec(memory_space=pltpu.VMEM)
    return pl.pallas_call(
        attend_back_kernel,
        grid_spec=pltpu.PrefetchScalarGridSpec(
            num_scalar_prefetch=2,
            grid=(1,),
            in_specs=[vmem] * 7,
            out_specs=[vmem, vmem],
            scratch_shapes=[
                pltpu.VMEM((total, HD), jnp.bfloat16),
                pltpu.VMEM((total, HD), jnp.bfloat16),
                pltpu.VMEM((HD, total), jnp.bfloat16),
                pltpu.VMEM((3 * HD, total), jnp.float32),
            ],
        ),
        out_shape=[
            jax.ShapeDtypeStruct((parts, 3 * HD, part_rows), jnp.bfloat16),
            jax.ShapeDtypeStruct((3 * HD, BLOCK), jnp.float32),
        ],
        cost_estimate=pl.CostEstimate(
            flops=3 * total * total * HD,
            transcendentals=total * total // 4,
            bytes_accessed=8 << 20,
        ),
        compiler_params=pltpu.CompilerParams(vmem_limit_bytes=50 << 20),
        name="attend_back",
    )(slot_of, low_tile, grad_parts, packed, exact, log_norm, start_row, cosine, sine_table)


def start_of(position, seq_lengths):
    seq_ends = jnp.cumsum(seq_lengths)
    ends_before = seq_ends[:, None] <= position[None, :]
    return jnp.sum(jnp.where(ends_before, seq_lengths[:, None], 0), axis=0)


def rotary_tables(offset_in_seq):
    half_rot = ROT // 2
    freq_table = jnp.power(10000.0, -2.0 * jnp.arange(half_rot, dtype=jnp.float32) / ROT)
    angles = freq_table[:, None] * offset_in_seq.astype(jnp.float32)[None, :]
    return jnp.cos(angles), jnp.sin(angles)


def on_device_layer(*arrays):
    return on_device_heads(*arrays)


def on_device_heads(
    tokens,
    norm1_gain,
    norm1_bias,
    w_qkv,
    qkv_bias,
    w_out,
    norm2_gain,
    norm2_bias,
    w_gate,
    w_up,
    w_down,
    cotangent,
    seq_lengths,
    block_order,
):
    head_index = lax.axis_index("head")
    blk_index = lax.axis_index("blk")
    x_index, core_index = head_index // 2, head_index % 2
    z_index, y_index = blk_index // 2, blk_index % 2
    tok_rows, model_width = tokens.shape
    plane_rows = 8 * tok_rows
    total_rows = Z_PARTS * plane_rows
    row_block = model_width // (2 * Z_PARTS)
    chunk = 2 * row_block
    ff_half = w_gate.shape[1] // 2
    heads_width = Z_PARTS * HD

    qkv_split = w_qkv.reshape(row_block, 3, Z_PARTS, 2, HD)
    qkv_low = qkv_split[:, :, :, 0].reshape(row_block, 3 * heads_width)
    qkv_high = qkv_split[:, :, :, 1].reshape(row_block, 3 * heads_width)
    first = y_index == 0
    qkv_even, qkv_odd = to_even_odd(
        jnp.where(first, qkv_low, qkv_high), jnp.where(first, qkv_high, qkv_low), y_index
    )
    out_split = w_out.reshape(Z_PARTS, 2, HD, row_block)
    out_low = out_split[:, 0].reshape(heads_width, row_block)
    out_high = out_split[:, 1].reshape(heads_width, row_block)
    out_even, out_odd = to_even_odd(
        jnp.where(first, out_low, out_high), jnp.where(first, out_high, out_low), y_index
    )

    def column_halves(weight):
        low, high = weight[:, :ff_half], weight[:, ff_half:]
        return to_even_odd(jnp.where(first, low, high), jnp.where(first, high, low), y_index)

    gate_own = jnp.concatenate(column_halves(w_gate), axis=0)
    up_own = jnp.concatenate(column_halves(w_up), axis=0)
    down_low, down_high = w_down[:ff_half], w_down[ff_half:]
    down_even, down_odd = to_even_odd(
        jnp.where(first, down_low, down_high), jnp.where(first, down_high, down_low), y_index
    )

    def both_ways(even, odd, axis):
        forward = ring_gather(even, 1)
        backward = ring_gather(odd, -1)
        pieces = [p for pair in zip(forward, backward) for p in pair]
        return jnp.concatenate(pieces, axis=axis)

    x_own = split_order(tokens, z_index, 1).astype(jnp.float32)
    gain_one = split_order(norm1_gain, z_index, 0)
    shift_one = split_order(norm1_bias, z_index, 0)
    gain_two = split_order(norm2_gain, z_index, 0)
    shift_two = split_order(norm2_bias, z_index, 0)
    norm1_out, unit_one, inv_one = normalize(x_own, gain_one, shift_one)
    norm1_all = gather_rows(norm1_out.astype(jnp.bfloat16))
    qkv_full = both_ways(qkv_even, qkv_odd, 0)
    out_full = both_ways(out_even, out_odd, 1)
    gate_full = jnp.concatenate(ring_gather(gate_own, 1), axis=0)
    up_full = jnp.concatenate(ring_gather(up_own, -1), axis=0)
    down_full = both_ways(down_even, down_odd, 1)

    slots = jnp.arange(Z_PARTS * 8, dtype=jnp.int32)
    step_z, flip = slots // 8, slots % 8
    owner = (
        ((x_index ^ ((flip // 2) % 2)) * 2 + (core_index ^ (flip // 4))) * (2 * Z_PARTS)
        + ((z_index - step_z + Z_PARTS) % Z_PARTS) * 2
        + (y_index ^ (flip % 2))
    )
    packed_block = jnp.sum(
        jnp.where(owner[:, None] == slots[None, :], block_order[None, :], 0), axis=1
    )
    slot_of = jnp.sum(
        jnp.where(packed_block[None, :] == slots[:, None], slots[None, :], 0), axis=1
    )
    plane_pos = (
        packed_block[:8, None] * BLOCK + jnp.arange(BLOCK, dtype=jnp.int32)[None, :]
    ).reshape(-1)
    plane_cos, plane_sin = rotary_tables(plane_pos - start_of(plane_pos, seq_lengths))
    all_pos = jnp.arange(total_rows, dtype=jnp.int32)
    all_start = start_of(all_pos, seq_lengths)
    all_cos, all_sin = rotary_tables(all_pos - all_start)
    low_tile = (
        start_of(
            jnp.arange(total_rows // QUERY_TILE, dtype=jnp.int32) * QUERY_TILE, seq_lengths
        )
        // KEY_TILE
    )
    start_row = all_start[None, :]

    bias_split = qkv_bias.reshape(3, Z_PARTS, 2, HD)
    bias_own = jnp.where(first, bias_split[:, :, 0], bias_split[:, :, 1]).reshape(-1)
    projected = (mm(qkv_full, norm1_all, 0, 1) + bias_own[:, None]).reshape(
        3, Z_PARTS, HD, plane_rows
    )
    half_rot = ROT // 2
    lead_part, tail_part = projected[:2, :, :half_rot], projected[:2, :, half_rot:ROT]
    rotated = jnp.concatenate(
        [
            lead_part * plane_cos - tail_part * plane_sin,
            tail_part * plane_cos + lead_part * plane_sin,
            projected[:2, :, ROT:],
        ],
        axis=2,
    )
    qkv_heads = jnp.concatenate([rotated, projected[2:]], axis=0).astype(jnp.bfloat16)
    qkv_heads = qkv_heads.transpose(1, 0, 2, 3).reshape(Z_PARTS, 3 * HD, plane_rows)
    qkv_parts = to_heads(qkv_heads, z_index)
    attn_parts, attn_exact, log_norm, packed = attend_heads(
        slot_of, low_tile, qkv_parts, start_row
    )
    attn_t = from_heads(attn_parts, z_index).reshape(heads_width, plane_rows)
    attn_own = scatter_rows(mm(attn_t, out_full, 0, 0))

    hidden = x_own + attn_own
    norm2_out, unit_two, inv_two = normalize(hidden, gain_two, shift_two)
    norm2_all = gather_rows(norm2_out.astype(jnp.bfloat16))
    cotangent_own = split_order(cotangent, z_index, 1)
    grad_all = gather_rows(cotangent_own)
    gate_val = mm(norm2_all, gate_full)
    up_val = mm(norm2_all, up_full)
    sigmoid_gate = jax.nn.sigmoid(gate_val)
    swish_val = gate_val * sigmoid_gate
    activ_b = (swish_val * up_val).astype(jnp.bfloat16)
    grad_activ = mm(grad_all, down_full, 1, 1)
    grad_up_b = (grad_activ * swish_val).astype(jnp.bfloat16)
    grad_gate_b = (
        grad_activ * up_val * sigmoid_gate * (1.0 + gate_val * (1.0 - sigmoid_gate))
    ).astype(jnp.bfloat16)
    grad_norm2 = scatter_rows(mm(grad_gate_b, gate_full, 1, 1) + mm(grad_up_b, up_full, 1, 1))

    def pieces_of(values, width, offset=0, size=None):
        size = width if size is None else size
        return [
            values[:, j * width + offset : j * width + offset + size] for j in range(Z_PARTS)
        ]

    down_sum_even = ring_scatter(
        [lambda p=p: mm(activ_b, p, 0, 0) for p in pieces_of(grad_all, chunk, 0, row_block)], 1
    )
    down_sum_odd = ring_scatter(
        [lambda p=p: mm(activ_b, p, 0, 0) for p in pieces_of(grad_all, chunk, row_block, row_block)], -1
    )
    down_parts = from_even_odd(down_sum_even, down_sum_odd, y_index)
    down_grad = jnp.concatenate(down_parts, axis=0)
    gate_sum = ring_scatter(
        [lambda p=p: mm(p, grad_gate_b, 0, 0) for p in pieces_of(norm2_all, chunk)], 1
    )
    up_sum = ring_scatter(
        [lambda p=p: mm(p, grad_up_b, 0, 0) for p in pieces_of(norm2_all, chunk)], -1
    )
    gate_grad = jnp.concatenate(
        from_even_odd(gate_sum[:row_block], gate_sum[row_block:], y_index), axis=1
    )
    up_grad = jnp.concatenate(
        from_even_odd(up_sum[:row_block], up_sum[row_block:], y_index), axis=1
    )

    grad_out = cotangent_own.astype(jnp.float32)
    grad_hidden = grad_out + normalize_back(grad_norm2, unit_two, inv_two, gain_two)
    branch_all = gather_rows(grad_hidden.astype(jnp.bfloat16))
    activ_late, branch_all = lax.optimization_barrier((activ_b, branch_all))
    mlp_own = scatter_rows(mm(activ_late, down_full))
    output = split_order((hidden + mlp_own).astype(jnp.bfloat16), z_index, 1)
    grad_attn = (
        mm(out_full, branch_all, 1, 1)
        .astype(jnp.bfloat16)
        .reshape(Z_PARTS, HD, plane_rows)
    )
    grad_parts = to_heads(grad_attn, z_index)
    proj_parts, bias_sums = attend_heads_back(
        slot_of, low_tile, grad_parts, packed, attn_exact, log_norm, start_row, all_cos, all_sin
    )
    bias_grad = jnp.sum(bias_sums, axis=1).reshape(3, HD)
    grad_proj = from_heads(proj_parts, z_index).reshape(Z_PARTS, 3, HD, plane_rows)
    grad_proj = grad_proj.transpose(1, 0, 2, 3).reshape(3 * heads_width, plane_rows)
    norm1_part = mm(grad_proj, qkv_full, 0, 1)
    grad_norm1 = scatter_rows(norm1_part)

    out_sum_even = ring_scatter(
        [lambda p=p: mm(attn_t, p) for p in pieces_of(branch_all, chunk, 0, row_block)], 1
    )
    out_sum_odd = ring_scatter(
        [lambda p=p: mm(attn_t, p) for p in pieces_of(branch_all, chunk, row_block, row_block)], -1
    )
    out_parts = from_even_odd(out_sum_even, out_sum_odd, y_index)
    out_grad = jnp.stack(
        [p.reshape(Z_PARTS, HD, row_block) for p in out_parts], axis=1
    ).reshape(w_out.shape)
    qkv_sum_even = ring_scatter(
        [lambda p=p: mm(p, grad_proj, 0, 1) for p in pieces_of(norm1_all, chunk, 0, row_block)], 1
    )
    qkv_sum_odd = ring_scatter(
        [lambda p=p: mm(p, grad_proj, 0, 1) for p in pieces_of(norm1_all, chunk, row_block, row_block)], -1
    )
    qkv_grad_parts = from_even_odd(qkv_sum_even, qkv_sum_odd, y_index)
    qkv_grad = jnp.stack(
        [p.reshape(row_block, 3, Z_PARTS, HD) for p in qkv_grad_parts], axis=3
    ).reshape(w_qkv.shape)

    input_grad = grad_hidden + normalize_back(grad_norm1, unit_one, inv_one, gain_one)
    sums = jnp.stack(
        [
            jnp.sum(grad_norm1 * unit_one, axis=0),
            jnp.sum(grad_norm1, axis=0),
            jnp.sum(grad_norm2 * unit_two, axis=0),
            jnp.sum(grad_norm2, axis=0),
        ],
        axis=0,
    )
    norm_sums = scatter_sums(
        split_order(sums, z_index, 1), x_index, core_index, z_index, y_index
    )
    return (
        output,
        split_order(input_grad, z_index, 1),
        norm_sums[0],
        norm_sums[1],
        qkv_grad,
        bias_grad,
        out_grad,
        norm_sums[2],
        norm_sums[3],
        gate_grad,
        up_grad,
        down_grad,
    )


def solution(mesh):
    placed = (
        P(("head", "blk"), None),
        P(),
        P(),
        P("blk", None, "head"),
        P(None, "head"),
        P("head", "blk"),
        P(),
        P(),
        P("blk", "head"),
        P("blk", "head"),
        P("head", "blk"),
        P(("head", "blk"), None),
        P(),
        P(),
    )
    heads_plan = mesh.shape["head"] == 4 and mesh.shape["blk"] == 2 * Z_PARTS
    return jax.shard_map(
        on_device_layer if heads_plan else on_device,
        mesh=mesh,
        in_specs=placed,
        out_specs=(
            P(("head", "blk"), None),
            P(("head", "blk"), None),
            P(("head", "blk")),
            P(("head", "blk")),
            P("blk", None, "head"),
            P(None, ("head", "blk")),
            P("head", "blk"),
            P(("head", "blk")),
            P(("head", "blk")),
            P("blk", "head"),
            P("blk", "head"),
            P("head", "blk"),
        ),
        check_vma=False,
    )
```
